32 devices in a mesh: lon: 4 (over y, core), lat: 8 (over z, x).
Axes of the slice: x: 2, y: 2, z: 4, core: 2. Of those that a mesh axis runs over, the one named last changes fastest.
Arguments:
- fields: bfloat16 [20, 16, 1024, 512], P(None, None, 'lat', 'lon'), may hold values from -16 to 16
- area: float32 [1024, 512], P('lat', 'lon'), may hold values from 0.2 to 5
- ocean: int32 [16, 1024, 512], P(None, 'lat', 'lon'), may hold values 0 or 1
- partner: int32 [512], replicated, may hold values from 0 to 511, as said below
- counted: int32 [512], replicated, may hold values from 0 to 1, as said below
Outputs:
- zonal_mean: float32 [20, 16, 1024], replicated
The draws below stay inside these ranges and needn't reach their ends.
Inputs may be any that keep to these rules, and one draw needn't show every extreme that they name: partner pairs the columns: partner[partner[i]] = i and partner[i] != i. Of each pair i, partner[i] exactly one has counted = 1.
All inputs are finite; a program needn't handle non-finite values. No bound on the sum of `ocean` on one device may be relied on, other than what follows from the above.
Results may differ from the reference program's by a relative error of at most 0.0003.
Values may be sent and summed in bfloat16 or wider, within the bound.
No kernel may reach another device: no remote copies, remote signals or barrier semaphores. Data moves between devices by JAX's collectives and lax.ppermute only.
A program may use at most 64 MiB of HBM per device.

```python
import math
import jax
import jax.numpy as jnp
from jax import lax

F = 20
LEV = 16
NLAT = 1024
NLON = 512


def fold_pairs(key):
    shuffled = jax.random.permutation(jax.random.fold_in(key, 7), NLON).astype(jnp.int32)
    firsts = shuffled[0::2]
    seconds = shuffled[1::2]
    partner = jnp.zeros((NLON,), jnp.int32).at[firsts].set(seconds).at[seconds].set(firsts)
    choose = jax.random.randint(jax.random.fold_in(key, 11), (NLON // 2,), 0, 2).astype(jnp.int32)
    counted = jnp.zeros((NLON,), jnp.int32).at[firsts].set(choose).at[seconds].set(1 - choose)
    return (partner, counted)


def draw_partner(key, part):
    return fold_pairs(key)[0]


def draw_counted(key, part):
    return fold_pairs(key)[1]


def draw_fields(key, part):
    key_offset = jax.random.fold_in(key, 1)
    key_noise = jax.random.fold_in(key, 2)
    offset = jax.random.normal(key_offset, (F, LEV, NLAT, 1), jnp.float32)
    spread = 1.5
    noise = jax.random.normal(key_noise, (F, LEV, NLAT, NLON), jnp.float32)
    return jnp.clip(offset + spread * noise, -16.0, 16.0).astype(jnp.bfloat16)


def set_ends(entries, stream_key, smallest, high):
    index_at = [jax.random.randint(jax.random.fold_in(stream_key, axis), (), 0, length) for axis, length in enumerate(entries.shape)]
    widest = entries.shape.index(max(entries.shape))
    beside = index_at[:widest] + [(index_at[widest] + 1) % entries.shape[widest]] + index_at[widest + 1:]
    return entries.at[tuple(index_at)].set(smallest).at[tuple(beside)].set(high)


def steps_of(key, shape, cuts, smallest, top_value):
    factor_of, own = 1.0, jax.random.fold_in(key, 6)
    for position, parts in cuts:
        draws = jnp.exp(jax.random.uniform(jax.random.fold_in(own, position), (parts,), jnp.float32, smallest / len(cuts), top_value / len(cuts)))
        factor_of = factor_of * jnp.repeat(draws, shape[position] // parts).reshape([-1 if axis == position else 1 for axis in range(len(shape))])
    return factor_of


def setup_inputs(seed: int = 0) -> dict:
    streams_of = jax.random.split(jax.random.key(seed), 6)
    fields = draw_fields(jax.random.fold_in(streams_of[5], 71), 0)
    area = jnp.clip(jnp.exp(math.log(5.0) - 3.218876 * jax.random.uniform(streams_of[1], (NLAT, NLON), jnp.float32) ** steps_of(streams_of[1], (NLAT, NLON), ((0, 8), (1, 4)), -0.2, 0.2)), 0.2, 5.0)
    ocean = set_ends((jax.random.randint(streams_of[2], (LEV, NLAT, NLON), 0, 4) < 3).astype(jnp.int32), jax.random.fold_in(streams_of[2], 1), 0, 1)
    partner = draw_partner(jax.random.fold_in(streams_of[5], 71), 0)
    counted = draw_counted(jax.random.fold_in(streams_of[5], 71), 0)
    return dict(fields=fields, area=area, ocean=ocean, partner=partner, counted=counted)


def reference(fields, area, ocean, partner, counted):
    row_index = jnp.arange(NLAT)[:, None]
    counted_weight = jnp.where(row_index == NLAT - 1, counted.astype(jnp.float32)[None, :], jnp.float32(1.0))
    cell_weight = counted_weight * area
    oceanic = ocean.astype(jnp.float32)
    weight = cell_weight[None] * oceanic
    row_weight = jnp.sum(cell_weight[None] * (oceanic + 0.05), axis=-1)
    fold_values = fields[:, :, NLAT - 1, :].astype(jnp.float32)
    merged = 0.5 * (fold_values + jnp.take(fold_values, partner, axis=2))

    def per_field(items):
        one_field, merged_row = items
        sums = jnp.sum(one_field.astype(jnp.float32) * weight, axis=-1)
        fold_sum = jnp.sum(merged_row * weight[:, NLAT - 1, :], axis=-1)
        return sums.at[:, NLAT - 1].set(fold_sum)

    row_sum = lax.map(per_field, (fields, merged))
    return row_sum / row_weight[None]
```

```python
import jax
import jax.numpy as jnp
from jax import lax
from jax.sharding import PartitionSpec as P


def bits_of(size):
    if size & (size - 1):
        raise ValueError("uneven axis")
    return [1 << k for k in range(size.bit_length() - 1)]


def exchange(value, axis, bit):
    size = lax.axis_size(axis)
    return lax.ppermute(value, axis, [(i, i ^ bit) for i in range(size)])


def per_device(fields, area, ocean, partner, counted):
    lon_size, lat_size = lax.axis_size("lon"), lax.axis_size("lat")
    my_lon, my_lat = lax.axis_index("lon"), lax.axis_index("lat")
    count, levels, lat_rows, lon_cols = fields.shape
    rows = count * levels
    offset = my_lon * lon_cols
    own_partner = lax.dynamic_slice_in_dim(partner, offset, lon_cols, 0)
    own_counted = lax.dynamic_slice_in_dim(counted, offset, lon_cols, 0)
    on_top = my_lat == lat_size - 1
    fold_row = jnp.logical_and(on_top, jnp.arange(lat_rows)[:, None] == lat_rows - 1)
    counted_weight = jnp.where(fold_row, own_counted.astype(jnp.float32)[None, :], jnp.float32(1.0))

    half_own = (0.5 * own_counted.astype(jnp.float32) * area[lat_rows - 1])[None] * ocean[:, lat_rows - 1, :].astype(jnp.float32)
    halves = half_own[None]
    for bit in bits_of(lon_size):
        halves = jnp.concatenate([halves, exchange(halves, "lon", bit)], axis=0)
    slot = jnp.bitwise_xor(own_partner // lon_cols, my_lon)
    flat = halves.transpose(1, 0, 2).reshape(levels, lon_size * lon_cols)
    from_partner = jnp.take(flat, slot * lon_cols + own_partner % lon_cols, axis=1)

    cell_weight = counted_weight * area
    oceanic = ocean.astype(jnp.float32)
    weight = cell_weight[None] * oceanic
    row_weight = jnp.sum(cell_weight[None] * (oceanic + 0.05), axis=-1)
    last_weight = jnp.where(on_top, half_own + from_partner, weight[:, lat_rows - 1, :])
    joined = jnp.concatenate([weight[:, : lat_rows - 1, :], last_weight[:, None, :]], axis=1)
    row_sum = jnp.sum(fields.astype(jnp.float32) * joined[None], axis=-1)

    part = row_sum.reshape(rows, lat_rows)
    start = jnp.int32(0)
    for bit in bits_of(lon_size):
        half = part.shape[0] // 2
        upper = jnp.bitwise_and(my_lon, bit) != 0
        keep = jnp.where(upper, part[half:], part[:half])
        send = jnp.where(upper, part[:half], part[half:])
        got = exchange(jnp.concatenate([send, row_weight], axis=0), "lon", bit)
        part = keep + got[:half]
        row_weight = row_weight + got[half:]
        start = start + jnp.where(upper, half, 0)
    chunk = part.shape[0]
    divisor = lax.dynamic_slice_in_dim(jnp.tile(row_weight, (count, 1)), start, chunk, 0)
    gathered = (part / divisor)[None]

    for bit in reversed(bits_of(lat_size)):
        gathered = jnp.concatenate([gathered, exchange(gathered, "lat", bit)], axis=0)
    for bit in reversed(bits_of(lon_size)):
        gathered = jnp.concatenate([gathered, exchange(gathered, "lon", bit)], axis=0)
    out = gathered
    axes_bits = [("lon", b) for b in bits_of(lon_size)] + [("lat", b) for b in bits_of(lat_size)]
    out = out.reshape((2,) * len(axes_bits) + out.shape[1:])
    for place, (axis, bit) in enumerate(axes_bits):
        me = my_lon if axis == "lon" else my_lat
        out = jnp.where(jnp.bitwise_and(me, bit) != 0, jnp.flip(out, place), out)
    n_lon, n_lat = len(bits_of(lon_size)), len(bits_of(lat_size))
    order = list(range(n_lon)) + [n_lon + n_lat] + list(reversed(range(n_lon, n_lon + n_lat))) + [n_lon + n_lat + 1]
    out = out.transpose(order).reshape(count, levels, lat_size * lat_rows)
    return out


def solution(mesh):
    in_specs = (P(None, None, "lat", "lon"), P("lat", "lon"), P(None, "lat", "lon"), P(), P())
    out_specs = P()
    return jax.shard_map(
        per_device, mesh=mesh, in_specs=in_specs, out_specs=out_specs, check_vma=False
    )
```

```python
import functools

import jax
import jax.numpy as jnp
from jax import lax
from jax.experimental import pallas as pl
from jax.experimental.pallas import tpu as pltpu
from jax.sharding import PartitionSpec as P

F32 = jnp.float32
VMEM = pltpu.VMEM


def bits_of(size):
    if size & (size - 1):
        raise ValueError("uneven axis")
    return [1 << k for k in range(size.bit_length() - 1)]


def exchange(value, axis, bit):
    size = lax.axis_size(axis)
    return lax.ppermute(value, axis, [(i, i ^ bit) for i in range(size)])


def own_columns(ref, cols):
    offset = pl.multiple_of(lax.axis_index("lon") * cols, cols)
    return ref[:, pl.ds(offset, cols)]


def on_top():
    return lax.axis_index("lat") == lax.axis_size("lat") - 1


def half_kernel(area_ref, ocean_ref, counted_ref, half_ref):
    cols = area_ref.shape[1]
    base = 0.5 * own_columns(counted_ref, cols).astype(F32) * area_ref[7:8, :]
    half_ref[...] = base * ocean_ref[:, 7, :].astype(F32)


def fold_halves(area, ocean, counted):
    levels, rows, cols = ocean.shape
    last = rows // 8 - 1
    return pl.pallas_call(
        half_kernel,
        grid=(1,),
        in_specs=[
            pl.BlockSpec((8, cols), lambda i: (last, 0)),
            pl.BlockSpec((levels, 8, cols), lambda i: (0, last, 0)),
            pl.BlockSpec(counted.shape, lambda i: (0, 0)),
        ],
        out_specs=pl.BlockSpec((levels, cols), lambda i: (0, 0)),
        out_shape=jax.ShapeDtypeStruct((levels, cols), F32),
        name="fold_halves",
    )(area, ocean, counted)


def weight_kernel(area_ref, ocean_ref, counted_ref, weight_ref, total_ref):
    levels, rows, cols = ocean_ref.shape
    counted = own_columns(counted_ref, cols).astype(F32)
    row = lax.broadcasted_iota(jnp.int32, (rows, cols), 0)
    fold = jnp.logical_and(row == rows - 1, on_top())
    cell = jnp.where(fold, counted, F32(1.0)) * area_ref[...]
    weight_ref[...] = cell[None] * ocean_ref[...].astype(F32)
    small = 0.05 * jnp.sum(cell.T, axis=0, keepdims=True)
    for level in range(levels):
        turned = weight_ref[level].T
        total_ref[level : level + 1, :] = jnp.sum(turned, axis=0, keepdims=True) + small


def weights_of(area, ocean, counted):
    levels, rows, cols = ocean.shape
    return pl.pallas_call(
        weight_kernel,
        out_shape=(
            jax.ShapeDtypeStruct((levels, rows, cols), F32),
            jax.ShapeDtypeStruct((levels, rows), F32),
        ),
        name="cell_weights",
    )(area, ocean, counted)


def sums_kernel(fields_ref, weight_ref, halves_ref, partner_ref, out_ref, turned_ref, acc_ref):
    step = pl.program_id(0)
    per_step, levels, rows, cols = fields_ref.shape

    @pl.when(step == 0)
    def _():
        partner = own_columns(partner_ref, cols)
        slot = jnp.bitwise_xor(partner // cols, lax.axis_index("lon"))
        lane = jnp.broadcast_to(partner % cols, (levels, cols))
        extra = jnp.zeros((levels, cols), F32)
        for k in range(halves_ref.shape[0]):
            picked = jnp.take_along_axis(halves_ref[k], lane, axis=1)
            extra = jnp.where(slot == k, picked, extra)
        last = lax.broadcasted_iota(jnp.int32, (8, cols), 0) == 7
        fold = jnp.logical_and(last, on_top())
        for level in range(levels):
            tail = weight_ref[level, rows - 8 :, :]
            tail = jnp.where(fold, 0.5 * tail + extra[level : level + 1, :], tail)
            whole = jnp.concatenate([weight_ref[level, : rows - 8, :], tail], axis=0)
            turned_ref[level] = whole.T

    for f in range(per_step):
        for level in range(levels):
            turned = fields_ref[f, level].T.astype(F32) * turned_ref[level]
            acc = jnp.sum(turned.reshape(cols // 8, 8, rows), axis=0)
            place = ((step * per_step + f) * levels + level) * 8
            acc_ref[pl.ds(pl.multiple_of(place, 8), 8), :] = acc

    @pl.when(step == pl.num_programs(0) - 1)
    def _():
        for group in range(out_ref.shape[0] // 8):
            total = acc_ref[pl.ds(group * 64, 8, stride=8), :]
            for s in range(1, 8):
                total = total + acc_ref[pl.ds(group * 64 + s, 8, stride=8), :]
            out_ref[group * 8 : group * 8 + 8, :] = total


def row_sums(fields, weight, halves, partner, per_step=2):
    count, levels, rows, cols = fields.shape
    return pl.pallas_call(
        sums_kernel,
        grid=(count // per_step,),
        in_specs=[
            pl.BlockSpec((per_step, levels, rows, cols), lambda i: (i, 0, 0, 0)),
            pl.BlockSpec(memory_space=VMEM),
            pl.BlockSpec(memory_space=VMEM),
            pl.BlockSpec(memory_space=VMEM),
        ],
        out_specs=pl.BlockSpec((count * levels, rows), lambda i: (0, 0)),
        out_shape=jax.ShapeDtypeStruct((count * levels, rows), F32),
        scratch_shapes=[
            pltpu.VMEM((levels, cols, rows), F32),
            pltpu.VMEM((count * levels * 8, rows), F32),
        ],
        name="row_sums",
    )(fields, weight, halves, partner)


def per_device(fields, area, ocean, partner, counted):
    lon_size, lat_size = lax.axis_size("lon"), lax.axis_size("lat")
    my_lon, my_lat = lax.axis_index("lon"), lax.axis_index("lat")
    count, levels, lat_rows, lon_cols = fields.shape
    partner, counted = partner[None], counted[None]

    halves = fold_halves(area, ocean, counted)[None]
    for bit in bits_of(lon_size):
        halves = jnp.concatenate([halves, exchange(halves, "lon", bit)], axis=0)
    weight, row_weight = weights_of(area, ocean, counted)
    part = row_sums(fields, weight, halves, partner)

    start = jnp.int32(0)
    for bit in bits_of(lon_size):
        half = part.shape[0] // 2
        upper = jnp.bitwise_and(my_lon, bit) != 0
        keep = jnp.where(upper, part[half:], part[:half])
        send = jnp.where(upper, part[:half], part[half:])
        got = exchange(jnp.concatenate([send, row_weight], axis=0), "lon", bit)
        part = keep + got[:half]
        row_weight = row_weight + got[half:]
        start = start + jnp.where(upper, half, 0)
    chunk = part.shape[0]
    divisor = lax.dynamic_slice_in_dim(jnp.tile(row_weight, (count, 1)), start, chunk, 0)
    gathered = (part / divisor)[None]

    for bit in reversed(bits_of(lat_size)):
        gathered = jnp.concatenate([gathered, exchange(gathered, "lat", bit)], axis=0)
    for bit in reversed(bits_of(lon_size)):
        gathered = jnp.concatenate([gathered, exchange(gathered, "lon", bit)], axis=0)
    out = gathered
    axes_bits = [("lon", b) for b in bits_of(lon_size)] + [("lat", b) for b in bits_of(lat_size)]
    out = out.reshape((2,) * len(axes_bits) + out.shape[1:])
    for place, (axis, bit) in enumerate(axes_bits):
        me = my_lon if axis == "lon" else my_lat
        out = jnp.where(jnp.bitwise_and(me, bit) != 0, jnp.flip(out, place), out)
    n_lon, n_lat = len(bits_of(lon_size)), len(bits_of(lat_size))
    order = list(range(n_lon)) + [n_lon + n_lat] + list(reversed(range(n_lon, n_lon + n_lat))) + [n_lon + n_lat + 1]
    out = out.transpose(order).reshape(count, levels, lat_size * lat_rows)
    return out


def solution(mesh):
    in_specs = (P(None, None, "lat", "lon"), P("lat", "lon"), P(None, "lat", "lon"), P(), P())
    out_specs = P()
    return jax.shard_map(
        per_device, mesh=mesh, in_specs=in_specs, out_specs=out_specs, check_vma=False
    )
```

```python
import functools

import jax
import jax.numpy as jnp
from jax import lax
from jax.experimental import pallas as pl
from jax.experimental.pallas import tpu as pltpu
from jax.sharding import PartitionSpec as P

F32 = jnp.float32
VMEM = pltpu.VMEM
MIB = 1 << 20


def params(mib):
    return pltpu.CompilerParams(vmem_limit_bytes=mib * MIB)


def bits_of(size):
    if size & (size - 1):
        raise ValueError("uneven axis")
    return [1 << k for k in range(size.bit_length() - 1)]


def exchange(value, axis, bit):
    size = lax.axis_size(axis)
    return lax.ppermute(value, axis, [(i, i ^ bit) for i in range(size)])


def own_columns(ref, cols):
    offset = pl.multiple_of(lax.axis_index("lon") * cols, cols)
    return ref[:, pl.ds(offset, cols)]


def on_top():
    return lax.axis_index("lat") == lax.axis_size("lat") - 1


def half_kernel(area_ref, ocean_ref, counted_ref, half_ref):
    cols = area_ref.shape[1]
    base = 0.5 * own_columns(counted_ref, cols).astype(F32) * area_ref[7:8, :]
    half_ref[...] = base * ocean_ref[:, 7, :].astype(F32)


def fold_halves(area, ocean, counted):
    levels, rows, cols = ocean.shape
    last = rows // 8 - 1
    return pl.pallas_call(
        half_kernel,
        grid=(1,),
        in_specs=[
            pl.BlockSpec((8, cols), lambda i: (last, 0)),
            pl.BlockSpec((levels, 8, cols), lambda i: (0, last, 0)),
            pl.BlockSpec(counted.shape, lambda i: (0, 0)),
        ],
        out_specs=pl.BlockSpec((levels, cols), lambda i: (0, 0)),
        out_shape=jax.ShapeDtypeStruct((levels, cols), F32),
        compiler_params=params(2),
        name="fold_halves",
    )(area, ocean, counted)


def weight_kernel(area_ref, ocean_ref, counted_ref, weight_ref, total_ref):
    levels, rows, cols = ocean_ref.shape
    counted = own_columns(counted_ref, cols).astype(F32)
    row = lax.broadcasted_iota(jnp.int32, (rows, cols), 0)
    fold = jnp.logical_and(row == rows - 1, on_top())
    cell = jnp.where(fold, counted, F32(1.0)) * area_ref[...]
    small = 0.05 * jnp.sum(cell.T, axis=0, keepdims=True)
    for level in range(levels):
        weight = cell * ocean_ref[level].astype(F32)
        weight_ref[level] = weight
        total_ref[level : level + 1, :] = jnp.sum(weight.T, axis=0, keepdims=True) + small


def weights_of(area, ocean, counted):
    levels, rows, cols = ocean.shape
    return pl.pallas_call(
        weight_kernel,
        in_specs=[pl.BlockSpec(memory_space=VMEM)] * 3,
        out_specs=[pl.BlockSpec(memory_space=VMEM)] * 2,
        out_shape=(
            jax.ShapeDtypeStruct((levels, rows, cols), F32),
            jax.ShapeDtypeStruct((levels, rows), F32),
        ),
        compiler_params=params(4),
        name="cell_weights",
    )(area, ocean, counted)


def sums_kernel(fields_ref, weight_ref, total_ref, halves_ref, partner_ref, keep_ref, send_ref, turned_ref, acc_ref, extra_ref):
    count, levels, rows, cols = fields_ref.shape
    partner = own_columns(partner_ref, cols)
    slot = jnp.bitwise_xor(partner // cols, lax.axis_index("lon"))
    lane = jnp.broadcast_to(partner % cols, (levels, cols))
    extra = jnp.zeros((levels, cols), F32)
    for k in range(halves_ref.shape[0]):
        picked = jnp.take_along_axis(halves_ref[k], lane, axis=1)
        extra = jnp.where(slot == k, picked, extra)
    extra_ref[...] = extra
    last = lax.broadcasted_iota(jnp.int32, (8, cols), 0) == 7
    fold = jnp.logical_and(last, on_top())

    per_trip = 4

    def trip(t, carry):
        for k in range(per_trip):
            level = t * per_trip + k
            tail = weight_ref[level, rows - 8 :, :]
            tail = jnp.where(fold, 0.5 * tail + extra_ref[pl.ds(level, 1), :], tail)
            whole = jnp.concatenate([weight_ref[level, : rows - 8, :], tail], axis=0)
            turned_ref[k] = whole.T
        for k in range(per_trip):
            level = t * per_trip + k
            for f in range(count):
                turned = fields_ref[f, level].T.astype(F32) * turned_ref[k]
                acc = jnp.sum(turned.reshape(cols // 8, 8, rows), axis=0)
                place = pl.multiple_of((f * levels + level) * 8, 8)
                acc_ref[pl.ds(place, 8), :] = acc
        return carry

    lax.fori_loop(0, levels // per_trip, trip, 0)
    half = count * levels // 2
    mine = jnp.bitwise_and(lax.axis_index("lon"), 1)
    for ref, side in ((keep_ref, mine), (send_ref, 1 - mine)):
        base = side * (half * 8)
        for group in range(half // 8):
            total = acc_ref[pl.ds(base + group * 64, 8, stride=8), :]
            for s in range(1, 8):
                total = total + acc_ref[pl.ds(base + group * 64 + s, 8, stride=8), :]
            ref[group * 8 : group * 8 + 8, :] = total
    send_ref[half:, :] = total_ref[...]


def row_sums(fields, weight, total, halves, partner):
    count, levels, rows, cols = fields.shape
    half = count * levels // 2
    return pl.pallas_call(
        sums_kernel,
        in_specs=[pl.BlockSpec(memory_space=VMEM)] * 5,
        out_specs=[pl.BlockSpec(memory_space=VMEM)] * 2,
        out_shape=(
            jax.ShapeDtypeStruct((half, rows), F32),
            jax.ShapeDtypeStruct((half + levels, rows), F32),
        ),
        scratch_shapes=[
            pltpu.VMEM((4, cols, rows), F32),
            pltpu.VMEM((count * levels * 8, rows), F32),
            pltpu.VMEM((levels, cols), F32),
        ],
        compiler_params=params(16),
        name="row_sums",
    )(fields, weight, total, halves, partner)


def gather_steps(lon_size, lat_size):
    ybits = bits_of(lon_size)[1:]
    lat_bits = bits_of(lat_size)
    xbits, zbits = lat_bits[: len(ybits)], lat_bits[len(ybits) :]
    steps = [((0, b), (0, b)) for b in reversed(zbits)]
    pairs = list(zip(xbits, ybits))
    steps += [((0, x), (y, 0)) for x, y in pairs]
    steps += [((y, 0), (0, x)) for x, y in pairs]
    steps += [((y, 0), (y, 0)) for y in ybits[len(pairs) :]]
    return steps


def joint_exchange(value, step, lon_size, lat_size):
    pairs = []
    for lon in range(lon_size):
        for lat in range(lat_size):
            dlon, dlat = step[lon & 1]
            pairs.append((lon * lat_size + lat, (lon ^ dlon) * lat_size + (lat ^ dlat)))
    return lax.ppermute(value, ("lon", "lat"), pairs)


def place_kernel(steps, lon_bits, rows, other, *refs):
    slots_ref, out_ref, sems = refs[0], refs[-2], refs[-1]
    slots, chunk, lanes = slots_ref.shape
    owner_lon = jnp.bitwise_xor(lax.axis_index("lon"), other)
    core = jnp.bitwise_and(owner_lon, 1)
    my_lat = lax.axis_index("lat")
    copies = []
    for s in range(slots):
        masks = [[0, 0], [0, 0]]
        for k, step in enumerate(steps):
            if s >> k & 1:
                for c in range(2):
                    masks[c][0] ^= step[c][0]
                    masks[c][1] ^= step[c][1]
        lon = jnp.bitwise_xor(owner_lon, jnp.where(core == 0, masks[0][0], masks[1][0]))
        lat = jnp.bitwise_xor(my_lat, jnp.where(core == 0, masks[0][1], masks[1][1]))
        row = jnp.int32(0)
        for k in range(lon_bits):
            row = row + jnp.bitwise_and(lon >> k, 1) * (rows >> (k + 1))
        dst = out_ref.at[pl.ds(pl.multiple_of(row, 8), chunk), pl.ds(pl.multiple_of(lat * lanes, lanes), lanes)]
        copy = pltpu.make_async_copy(slots_ref.at[s], dst, sems.at[s])
        copy.start()
        copies.append(copy)
    for copy in copies:
        copy.wait()


def place(slots, into, steps, lon_bits, shape, other):
    rows = shape[0]
    args = (slots,) if into is None else (slots, into)
    specs = [pl.BlockSpec(memory_space=VMEM), pl.BlockSpec(memory_space=pl.ANY)]
    return pl.pallas_call(
        functools.partial(place_kernel, steps, lon_bits, rows, other),
        in_specs=specs[: len(args)],
        out_specs=pl.BlockSpec(memory_space=pl.ANY),
        out_shape=jax.ShapeDtypeStruct(shape, F32),
        scratch_shapes=[pltpu.SemaphoreType.DMA((slots.shape[0],))],
        input_output_aliases={} if into is None else {1: 0},
        compiler_params=params(4),
        name=f"place_{other}",
    )(*args)


def per_device(fields, area, ocean, partner, counted):
    lon_size, lat_size = lax.axis_size("lon"), lax.axis_size("lat")
    my_lon = lax.axis_index("lon")
    count, levels, lat_rows, lon_cols = fields.shape
    rows = count * levels
    lon_bits = bits_of(lon_size)
    partner, counted = partner[None], counted[None]

    halves = fold_halves(area, ocean, counted)[None]
    for bit in lon_bits:
        halves = jnp.concatenate([halves, exchange(halves, "lon", bit)], axis=0)
    weight, total = weights_of(area, ocean, counted)
    keep, send = row_sums(fields, weight, total, halves, partner)

    start = jnp.int32(0)
    for k, bit in enumerate(lon_bits):
        half = keep.shape[0]
        got = exchange(send, "lon", bit)
        part = keep + got[:half]
        total = total + got[half:]
        start = start + jnp.where(jnp.bitwise_and(my_lon, bit) != 0, half, 0)
        if k + 1 < len(lon_bits):
            upper = jnp.bitwise_and(my_lon, lon_bits[k + 1]) != 0
            low, high = part[: half // 2], part[half // 2 :]
            keep = jnp.where(upper, high, low)
            send = jnp.concatenate([jnp.where(upper, low, high), total], axis=0)
    chunk = part.shape[0]
    divisor = lax.dynamic_slice_in_dim(jnp.tile(total, (count, 1)), start, chunk, 0)
    slots = (part / divisor)[None]

    steps = gather_steps(lon_size, lat_size)
    for step in steps:
        slots = jnp.concatenate([slots, joint_exchange(slots, step, lon_size, lat_size)], axis=0)
    others = exchange(slots, "lon", 1)
    shape = (rows, lat_size * lat_rows)
    out = place(slots, None, steps, len(lon_bits), shape, 0)
    out = place(others, out, steps, len(lon_bits), shape, 1)
    return out.reshape(count, levels, lat_size * lat_rows)


def solution(mesh):
    in_specs = (P(None, None, "lat", "lon"), P("lat", "lon"), P(None, "lat", "lon"), P(), P())
    out_specs = P()
    return jax.shard_map(
        per_device, mesh=mesh, in_specs=in_specs, out_specs=out_specs, check_vma=False
    )
```

```python
import functools

import jax
import jax.numpy as jnp
from jax import lax
from jax.experimental import pallas as pl
from jax.experimental.pallas import tpu as pltpu
from jax.sharding import PartitionSpec as P

F32 = jnp.float32
VMEM = pltpu.VMEM
MIB = 1 << 20


def params(mib):
    return pltpu.CompilerParams(vmem_limit_bytes=mib * MIB)


def bits_of(size):
    if size & (size - 1):
        raise ValueError("uneven axis")
    return [1 << k for k in range(size.bit_length() - 1)]


def exchange(value, axis, bit):
    size = lax.axis_size(axis)
    return lax.ppermute(value, axis, [(i, i ^ bit) for i in range(size)])


def own_columns(ref, cols):
    offset = pl.multiple_of(lax.axis_index("lon") * cols, cols)
    return ref[:, pl.ds(offset, cols)]


def on_top():
    return lax.axis_index("lat") == lax.axis_size("lat") - 1


def pass_kernel(in_ref, out_ref):
    out_ref[...] = in_ref[:, in_ref.shape[1] - 1, :]


def last_row(value):
    levels, _, cols = value.shape
    return pl.pallas_call(
        pass_kernel,
        in_specs=[pl.BlockSpec(memory_space=VMEM)],
        out_specs=pl.BlockSpec(memory_space=VMEM),
        out_shape=jax.ShapeDtypeStruct((levels, cols), value.dtype),
        compiler_params=params(1),
        cost_estimate=pl.CostEstimate(flops=4_000_000_000, bytes_accessed=100, transcendentals=0),
        name="last_row",
    )(value)


def weight_kernel(area_ref, ocean_ref, counted_ref, weight_ref, total_ref):
    levels, rows, cols = ocean_ref.shape
    counted = own_columns(counted_ref, cols).astype(F32)
    row = lax.broadcasted_iota(jnp.int32, (rows, cols), 0)
    fold = jnp.logical_and(row == rows - 1, on_top())
    cell = jnp.where(fold, counted, F32(1.0)) * area_ref[...]
    small = 0.05 * jnp.sum(cell.T, axis=0, keepdims=True)
    for level in range(levels):
        weight = cell * ocean_ref[level].astype(F32)
        weight_ref[level] = weight
        total_ref[level : level + 1, :] = jnp.sum(weight.T, axis=0, keepdims=True) + small


def weights_of(area, ocean, counted):
    levels, rows, cols = ocean.shape
    return pl.pallas_call(
        weight_kernel,
        in_specs=[pl.BlockSpec(memory_space=VMEM)] * 3,
        out_specs=[pl.BlockSpec(memory_space=VMEM)] * 2,
        out_shape=(
            jax.ShapeDtypeStruct((levels, rows, cols), F32),
            jax.ShapeDtypeStruct((levels, rows), F32),
        ),
        compiler_params=params(4),
        name="cell_weights",
    )(area, ocean, counted)


def sums_kernel(fields_ref, weight_ref, total_ref, cells_ref, partner_ref, counted_ref, keep_ref, send_ref, turned_ref, acc_ref, extra_ref):
    count, levels, rows, cols = fields_ref.shape
    partner = own_columns(partner_ref, cols)
    slot = jnp.bitwise_xor(partner // cols, lax.axis_index("lon"))
    lane = jnp.broadcast_to(partner % cols, (levels, cols))
    extra = jnp.zeros((levels, cols), F32)
    for k in range(cells_ref.shape[0]):
        picked = jnp.take_along_axis(cells_ref[k], lane, axis=1)
        extra = jnp.where(slot == k, picked, extra)
    extra_ref[...] = extra * (0.5 - 0.5 * own_columns(counted_ref, cols).astype(F32))
    last = lax.broadcasted_iota(jnp.int32, (8, cols), 0) == 7
    fold = jnp.logical_and(last, on_top())

    per_trip = 4

    def trip(t, carry):
        for k in range(per_trip):
            level = t * per_trip + k
            tail = weight_ref[level, rows - 8 :, :]
            tail = jnp.where(fold, 0.5 * tail + extra_ref[pl.ds(level, 1), :], tail)
            whole = jnp.concatenate([weight_ref[level, : rows - 8, :], tail], axis=0)
            turned_ref[k] = whole.T
        for k in range(per_trip):
            level = t * per_trip + k
            for f in range(count):
                turned = fields_ref[f, level].T.astype(F32) * turned_ref[k]
                acc = jnp.sum(turned.reshape(cols // 8, 8, rows), axis=0)
                place = pl.multiple_of((f * levels + level) * 8, 8)
                acc_ref[pl.ds(place, 8), :] = acc
        return carry

    lax.fori_loop(0, levels // per_trip, trip, 0)
    half = count * levels // 2
    mine = jnp.bitwise_and(lax.axis_index("lon"), 1)
    for ref, side in ((keep_ref, mine), (send_ref, 1 - mine)):
        base = side * (half * 8)
        for group in range(half // 8):
            total = acc_ref[pl.ds(base + group * 64, 8, stride=8), :]
            for s in range(1, 8):
                total = total + acc_ref[pl.ds(base + group * 64 + s, 8, stride=8), :]
            ref[group * 8 : group * 8 + 8, :] = total
    send_ref[half:, :] = total_ref[...]


def row_sums(fields, weight, total, cells, partner, counted):
    count, levels, rows, cols = fields.shape
    half = count * levels // 2
    return pl.pallas_call(
        sums_kernel,
        in_specs=[pl.BlockSpec(memory_space=VMEM)] * 6,
        out_specs=[pl.BlockSpec(memory_space=VMEM)] * 2,
        out_shape=(
            jax.ShapeDtypeStruct((half, rows), F32),
            jax.ShapeDtypeStruct((half + levels, rows), F32),
        ),
        scratch_shapes=[
            pltpu.VMEM((4, cols, rows), F32),
            pltpu.VMEM((count * levels * 8, rows), F32),
            pltpu.VMEM((levels, cols), F32),
        ],
        compiler_params=params(16),
        name="row_sums",
    )(fields, weight, total, cells, partner, counted)


def gather_steps(lon_size, lat_size):
    ybits = bits_of(lon_size)[1:]
    lat_bits = bits_of(lat_size)
    xbits, zbits = lat_bits[: len(ybits)], lat_bits[len(ybits) :]
    steps = [((0, b), (0, b)) for b in reversed(zbits)]
    pairs = list(zip(xbits, ybits))
    steps += [((0, x), (y, 0)) for x, y in pairs]
    steps += [((y, 0), (0, x)) for x, y in pairs]
    steps += [((y, 0), (y, 0)) for y in ybits[len(pairs) :]]
    return steps


def joint_exchange(value, step, lon_size, lat_size):
    pairs = []
    for lon in range(lon_size):
        for lat in range(lat_size):
            dlon, dlat = step[lon & 1]
            pairs.append((lon * lat_size + lat, (lon ^ dlon) * lat_size + (lat ^ dlat)))
    return lax.ppermute(value, ("lon", "lat"), pairs)


def place_kernel(steps, lon_bits, rows, other, *refs):
    slots_ref, out_ref, sems = refs[0], refs[-2], refs[-1]
    slots, chunk, lanes = slots_ref.shape
    owner_lon = jnp.bitwise_xor(lax.axis_index("lon"), other)
    core = jnp.bitwise_and(owner_lon, 1)
    my_lat = lax.axis_index("lat")
    copies = []
    for s in range(slots):
        masks = [[0, 0], [0, 0]]
        for k, step in enumerate(steps):
            if s >> k & 1:
                for c in range(2):
                    masks[c][0] ^= step[c][0]
                    masks[c][1] ^= step[c][1]
        lon = jnp.bitwise_xor(owner_lon, jnp.where(core == 0, masks[0][0], masks[1][0]))
        lat = jnp.bitwise_xor(my_lat, jnp.where(core == 0, masks[0][1], masks[1][1]))
        row = jnp.int32(0)
        for k in range(lon_bits):
            row = row + jnp.bitwise_and(lon >> k, 1) * (rows >> (k + 1))
        dst = out_ref.at[pl.ds(pl.multiple_of(row, 8), chunk), pl.ds(pl.multiple_of(lat * lanes, lanes), lanes)]
        copy = pltpu.make_async_copy(slots_ref.at[s], dst, sems.at[s])
        copy.start()
        copies.append(copy)
    for copy in copies:
        copy.wait()


def place(slots, into, steps, lon_bits, shape, other):
    rows = shape[0]
    args = (slots,) if into is None else (slots, into)
    specs = [pl.BlockSpec(memory_space=VMEM), pl.BlockSpec(memory_space=pl.ANY)]
    return pl.pallas_call(
        functools.partial(place_kernel, steps, lon_bits, rows, other),
        in_specs=specs[: len(args)],
        out_specs=pl.BlockSpec(memory_space=pl.ANY),
        out_shape=jax.ShapeDtypeStruct(shape, F32),
        scratch_shapes=[pltpu.SemaphoreType.DMA((slots.shape[0],))],
        input_output_aliases={} if into is None else {1: 0},
        compiler_params=params(4),
        name=f"place_{other}",
    )(*args)


def per_device(fields, area, ocean, partner, counted):
    lon_size, lat_size = lax.axis_size("lon"), lax.axis_size("lat")
    my_lon = lax.axis_index("lon")
    count, levels, lat_rows, lon_cols = fields.shape
    rows = count * levels
    lon_bits = bits_of(lon_size)
    partner, counted = partner[None], counted[None]

    cells = last_row(area[None, lat_rows - 8 :] * ocean[:, lat_rows - 8 :].astype(F32))[None]
    for bit in lon_bits:
        cells = jnp.concatenate([cells, exchange(cells, "lon", bit)], axis=0)
    weight, total = weights_of(area, ocean, counted)
    keep, send = row_sums(fields, weight, total, cells, partner, counted)

    start = jnp.int32(0)
    for k, bit in enumerate(lon_bits):
        half = keep.shape[0]
        got = exchange(send, "lon", bit)
        part = keep + got[:half]
        total = total + got[half:]
        start = start + jnp.where(jnp.bitwise_and(my_lon, bit) != 0, half, 0)
        if k + 1 < len(lon_bits):
            upper = jnp.bitwise_and(my_lon, lon_bits[k + 1]) != 0
            low, high = part[: half // 2], part[half // 2 :]
            keep = jnp.where(upper, high, low)
            send = jnp.concatenate([jnp.where(upper, low, high), total], axis=0)
    chunk = part.shape[0]
    divisor = lax.dynamic_slice_in_dim(jnp.tile(total, (count, 1)), start, chunk, 0)
    slots = (part / divisor)[None]

    steps = gather_steps(lon_size, lat_size)
    for step in steps:
        slots = jnp.concatenate([slots, joint_exchange(slots, step, lon_size, lat_size)], axis=0)
    others = exchange(slots, "lon", 1)
    shape = (rows, lat_size * lat_rows)
    out = place(slots, None, steps, len(lon_bits), shape, 0)
    out = place(others, out, steps, len(lon_bits), shape, 1)
    return out.reshape(count, levels, lat_size * lat_rows)


def solution(mesh):
    in_specs = (P(None, None, "lat", "lon"), P("lat", "lon"), P(None, "lat", "lon"), P(), P())
    out_specs = P()
    return jax.shard_map(
        per_device, mesh=mesh, in_specs=in_specs, out_specs=out_specs, check_vma=False
    )
```

```python
import functools

import jax
import jax.numpy as jnp
from jax import lax
from jax.experimental import pallas as pl
from jax.experimental.pallas import tpu as pltpu
from jax.sharding import PartitionSpec as P

F32 = jnp.float32
VMEM = pltpu.VMEM
MIB = 1 << 20
TOP = 32767.0
STEPS = 256.0
TINY = 2.0**-126


def params(mib):
    return pltpu.CompilerParams(vmem_limit_bytes=mib * MIB)


def bits_of(size):
    if size & (size - 1):
        raise ValueError("uneven axis")
    return [1 << k for k in range(size.bit_length() - 1)]


def exchange(value, axis, bit):
    size = lax.axis_size(axis)
    return lax.ppermute(value, axis, [(i, i ^ bit) for i in range(size)])


def own_columns(ref, cols):
    offset = pl.multiple_of(lax.axis_index("lon") * cols, cols)
    return ref[:, pl.ds(offset, cols)]


def on_top():
    return lax.axis_index("lat") == lax.axis_size("lat") - 1


def pass_kernel(in_ref, out_ref):
    out_ref[...] = in_ref[:, in_ref.shape[1] - 1, :]


def last_row(value):
    levels, _, cols = value.shape
    return pl.pallas_call(
        pass_kernel,
        in_specs=[pl.BlockSpec(memory_space=VMEM)],
        out_specs=pl.BlockSpec(memory_space=VMEM),
        out_shape=jax.ShapeDtypeStruct((levels, cols), value.dtype),
        compiler_params=params(1),
        cost_estimate=pl.CostEstimate(flops=4_000_000_000, bytes_accessed=100, transcendentals=0),
        name="last_row",
    )(value)


def weight_kernel(area_ref, ocean_ref, counted_ref, weight_ref, total_ref):
    levels, rows, cols = ocean_ref.shape
    counted = own_columns(counted_ref, cols).astype(F32)
    row = lax.broadcasted_iota(jnp.int32, (rows, cols), 0)
    fold = jnp.logical_and(row == rows - 1, on_top())
    cell = jnp.where(fold, counted, F32(1.0)) * area_ref[...]
    small = 0.05 * jnp.sum(cell.T, axis=0, keepdims=True)
    for level in range(levels):
        weight = cell * ocean_ref[level].astype(F32)
        weight_ref[level] = weight
        total_ref[level : level + 1, :] = jnp.sum(weight.T, axis=0, keepdims=True) + small


def weights_of(area, ocean, counted):
    levels, rows, cols = ocean.shape
    return pl.pallas_call(
        weight_kernel,
        in_specs=[pl.BlockSpec(memory_space=VMEM)] * 3,
        out_specs=[pl.BlockSpec(memory_space=VMEM)] * 2,
        out_shape=(
            jax.ShapeDtypeStruct((levels, rows, cols), F32),
            jax.ShapeDtypeStruct((levels, rows), F32),
        ),
        compiler_params=params(4),
        name="cell_weights",
    )(area, ocean, counted)


def sums_kernel(fields_ref, weight_ref, total_ref, cells_ref, partner_ref, counted_ref, keep_ref, send_ref, turned_ref, acc_ref, extra_ref):
    count, levels, rows, cols = fields_ref.shape
    partner = own_columns(partner_ref, cols)
    slot = jnp.bitwise_xor(partner // cols, lax.axis_index("lon"))
    lane = jnp.broadcast_to(partner % cols, (levels, cols))
    extra = jnp.zeros((levels, cols), F32)
    for k in range(cells_ref.shape[0]):
        picked = jnp.take_along_axis(cells_ref[k], lane, axis=1)
        extra = jnp.where(slot == k, picked, extra)
    extra_ref[...] = extra * (0.5 - 0.5 * own_columns(counted_ref, cols).astype(F32))
    last = lax.broadcasted_iota(jnp.int32, (8, cols), 0) == 7
    fold = jnp.logical_and(last, on_top())

    per_trip = 4

    def trip(t, carry):
        for k in range(per_trip):
            level = t * per_trip + k
            tail = weight_ref[level, rows - 8 :, :]
            tail = jnp.where(fold, 0.5 * tail + extra_ref[pl.ds(level, 1), :], tail)
            whole = jnp.concatenate([weight_ref[level, : rows - 8, :], tail], axis=0)
            turned_ref[k] = whole.T
        for k in range(per_trip):
            level = t * per_trip + k
            for f in range(count):
                turned = fields_ref[f, level].T.astype(F32) * turned_ref[k]
                acc = jnp.sum(turned.reshape(cols // 8, 8, rows), axis=0)
                place = pl.multiple_of((f * levels + level) * 8, 8)
                acc_ref[pl.ds(place, 8), :] = acc
        return carry

    lax.fori_loop(0, levels // per_trip, trip, 0)
    half = count * levels // 2
    mine = jnp.bitwise_and(lax.axis_index("lon"), 1)
    for ref, side in ((keep_ref, mine), (send_ref, 1 - mine)):
        base = side * (half * 8)
        for group in range(half // 8):
            total = acc_ref[pl.ds(base + group * 64, 8, stride=8), :]
            for s in range(1, 8):
                total = total + acc_ref[pl.ds(base + group * 64 + s, 8, stride=8), :]
            ref[group * 8 : group * 8 + 8, :] = total
    send_ref[half:, :] = total_ref[...]


def row_sums(fields, weight, total, cells, partner, counted):
    count, levels, rows, cols = fields.shape
    half = count * levels // 2
    return pl.pallas_call(
        sums_kernel,
        in_specs=[pl.BlockSpec(memory_space=VMEM)] * 6,
        out_specs=[pl.BlockSpec(memory_space=VMEM)] * 2,
        out_shape=(
            jax.ShapeDtypeStruct((half, rows), F32),
            jax.ShapeDtypeStruct((half + levels, rows), F32),
        ),
        scratch_shapes=[
            pltpu.VMEM((4, cols, rows), F32),
            pltpu.VMEM((count * levels * 8, rows), F32),
            pltpu.VMEM((levels, cols), F32),
        ],
        compiler_params=params(16),
        name="row_sums",
    )(fields, weight, total, cells, partner, counted)


def finish_kernel(keep_ref, got_ref, total_ref, code_ref, sum_ref):
    chunk, lanes = keep_ref.shape
    levels = total_ref.shape[0]
    bits = bits_of(lax.axis_size("lon"))
    lon = lax.axis_index("lon")
    start = jnp.int32(0)
    for k in range(len(bits)):
        start = start + jnp.bitwise_and(lon >> k, 1) * (chunk * len_ratio(bits, k))
    sum_ref[...] = total_ref[...] + got_ref[chunk:, :]
    most = jnp.zeros((8, lanes), F32)
    means = []
    for r in range(0, chunk, 8):
        level = pl.multiple_of(lax.rem(start + r, levels), 8)
        part = keep_ref[r : r + 8, :] + got_ref[r : r + 8, :]
        mean = part / sum_ref[pl.ds(level, 8), :]
        most = jnp.maximum(most, jnp.abs(mean))
        means.append(mean)
    most = jnp.maximum(jnp.max(most, axis=0, keepdims=True), TINY)
    power = jnp.minimum(jnp.ceil(jnp.log2(most) * STEPS) + 1.0, 127.0 * STEPS)
    scale = jnp.exp2(power * (1.0 / STEPS))
    for k, mean in enumerate(means):
        code = jnp.clip(jnp.round(mean / scale * TOP), -TOP, TOP)
        code_ref[0, 8 * k : 8 * k + 8, :] = code.astype(jnp.int32).astype(jnp.int16)
    power = jnp.broadcast_to(power, (8, lanes)).astype(jnp.int32)
    code_ref[0, chunk : chunk + 8, :] = power.astype(jnp.int16)


def len_ratio(bits, k):
    return 1 << (len(bits) - 1 - k)


def finish(keep, got, total):
    chunk, lanes = keep.shape
    return pl.pallas_call(
        finish_kernel,
        in_specs=[pl.BlockSpec(memory_space=VMEM)] * 3,
        out_specs=pl.BlockSpec(memory_space=VMEM),
        out_shape=jax.ShapeDtypeStruct((1, chunk + 8, lanes), jnp.int16),
        scratch_shapes=[pltpu.VMEM(total.shape, F32)],
        compiler_params=params(2),
        name="finish",
    )(keep, got, total)


def place_kernel(masks, rows, other, *refs):
    slots_ref, out_ref, mean_ref, sems = refs[0], refs[-3], refs[-2], refs[-1]
    slots, chunk, lanes = mean_ref.shape
    owner_lon = jnp.bitwise_xor(lax.axis_index("lon"), other)
    lon_bits = len(bits_of(lax.axis_size("lon")))
    copies = []
    for s in range(slots):
        power = slots_ref[s, chunk : chunk + 8, :].astype(jnp.int32).astype(F32)
        scale = jnp.exp2(power * (1.0 / STEPS)) * (1.0 / TOP)
        code = slots_ref[s, :chunk, :].astype(jnp.int32).astype(F32)
        mean_ref[s] = (code.reshape(chunk // 8, 8, lanes) * scale[None]).reshape(chunk, lanes)
        dlon, dlat = 0, 0
        for k, mask in enumerate(masks):
            if s >> k & 1:
                dlon, dlat = dlon ^ mask[0], dlat ^ mask[1]
        lon = jnp.bitwise_xor(owner_lon, dlon)
        lat = jnp.bitwise_xor(lax.axis_index("lat"), dlat)
        row = jnp.int32(0)
        for k in range(lon_bits):
            row = row + jnp.bitwise_and(lon >> k, 1) * (rows >> (k + 1))
        dst = out_ref.at[pl.ds(pl.multiple_of(row, 8), chunk), pl.ds(pl.multiple_of(lat * lanes, lanes), lanes)]
        copies.append(pltpu.make_async_copy(mean_ref.at[s], dst, sems.at[s]))
        if s:
            copies[s - 1].start()
    copies[-1].start()
    for copy in copies:
        copy.wait()


def place(slots, into, masks, shape, other):
    args = (slots,) if into is None else (slots, into)
    specs = [pl.BlockSpec(memory_space=VMEM), pl.BlockSpec(memory_space=pl.ANY)]
    count, chunk, lanes = slots.shape
    return pl.pallas_call(
        functools.partial(place_kernel, masks, shape[0], other),
        in_specs=specs[: len(args)],
        out_specs=pl.BlockSpec(memory_space=pl.ANY),
        out_shape=jax.ShapeDtypeStruct(shape, F32),
        scratch_shapes=[
            pltpu.VMEM((count, chunk - 8, lanes), F32),
            pltpu.SemaphoreType.DMA((count,)),
        ],
        input_output_aliases={} if into is None else {1: 0},
        compiler_params=params(4),
        name=f"place_{other}",
    )(*args)


def per_device(fields, area, ocean, partner, counted):
    lon_size, lat_size = lax.axis_size("lon"), lax.axis_size("lat")
    my_lon = lax.axis_index("lon")
    count, levels, lat_rows, lon_cols = fields.shape
    rows = count * levels
    lon_bits = bits_of(lon_size)
    partner, counted = partner[None], counted[None]

    cells = last_row(area[None, lat_rows - 8 :] * ocean[:, lat_rows - 8 :].astype(F32))[None]
    for bit in lon_bits:
        cells = jnp.concatenate([cells, exchange(cells, "lon", bit)], axis=0)
    weight, total = weights_of(area, ocean, counted)
    keep, send = row_sums(fields, weight, total, cells, partner, counted)

    for bit in lon_bits[1:]:
        half = keep.shape[0]
        got = exchange(send, "lon", bit >> 1)
        part = keep + got[:half]
        total = total + got[half:]
        upper = jnp.bitwise_and(my_lon, bit) != 0
        low, high = part[: half // 2], part[half // 2 :]
        keep = jnp.where(upper, high, low)
        send = jnp.concatenate([jnp.where(upper, low, high), total], axis=0)
    slots = finish(keep, exchange(send, "lon", lon_bits[-1]), total)

    masks = []
    for axis, bits in (("lat", bits_of(lat_size)), ("lon", lon_bits[1:])):
        for bit in reversed(bits):
            slots = jnp.concatenate([slots, exchange(slots, axis, bit)], axis=0)
            masks.append((0, bit) if axis == "lat" else (bit, 0))
    others = exchange(slots, "lon", 1)
    shape = (rows, lat_size * lat_rows)
    out = place(slots, None, masks, shape, 0)
    out = place(others, out, masks, shape, 1)
    return out.reshape(count, levels, lat_size * lat_rows)


def solution(mesh):
    in_specs = (P(None, None, "lat", "lon"), P("lat", "lon"), P(None, "lat", "lon"), P(), P())
    out_specs = P()
    return jax.shard_map(
        per_device, mesh=mesh, in_specs=in_specs, out_specs=out_specs, check_vma=False
    )
```

```python
import functools

import jax
import jax.numpy as jnp
from jax import lax
from jax.experimental import pallas as pl
from jax.experimental.pallas import tpu as pltpu
from jax.sharding import PartitionSpec as P

F32 = jnp.float32
VMEM = pltpu.VMEM
MIB = 1 << 20
TOP = 32767.0
STEPS = 256.0
TINY = 2.0**-126


def params(mib):
    return pltpu.CompilerParams(vmem_limit_bytes=mib * MIB)


def bits_of(size):
    if size & (size - 1):
        raise ValueError("uneven axis")
    return [1 << k for k in range(size.bit_length() - 1)]


def exchange(value, axis, bit):
    size = lax.axis_size(axis)
    return lax.ppermute(value, axis, [(i, i ^ bit) for i in range(size)])


def exchange_both(value, lat_bit, lon_bit):
    lons, lats = lax.axis_size("lon"), lax.axis_size("lat")
    pairs = [(i * lats + j, (i ^ lon_bit) * lats + (j ^ lat_bit)) for i in range(lons) for j in range(lats)]
    return lax.ppermute(value, ("lon", "lat"), pairs)


def own_columns(ref, cols):
    offset = pl.multiple_of(lax.axis_index("lon") * cols, cols)
    return ref[:, pl.ds(offset, cols)]


def on_top():
    return lax.axis_index("lat") == lax.axis_size("lat") - 1


def first_kernel(out_ref):
    out_ref[...] = jnp.zeros_like(out_ref)


def first():
    return pl.pallas_call(
        first_kernel,
        out_specs=pl.BlockSpec(memory_space=VMEM),
        out_shape=jax.ShapeDtypeStruct((8, 128), F32),
        compiler_params=params(1),
        cost_estimate=pl.CostEstimate(flops=4_000_000_000, bytes_accessed=100, transcendentals=0),
        name="first",
    )()


def weight_kernel(_, area_ref, ocean_ref, counted_ref, turned_ref, total_ref, cells_ref):
    levels, rows, cols = ocean_ref.shape
    counted = own_columns(counted_ref, cols).astype(F32)
    row = lax.broadcasted_iota(jnp.int32, (rows, cols), 0)
    fold = jnp.logical_and(row == rows - 1, on_top())
    cell = jnp.where(fold, counted, F32(1.0)) * area_ref[...]
    small = 0.05 * jnp.sum(cell.T, axis=0, keepdims=True)
    cells_ref[...] = area_ref[rows - 1 :, :] * ocean_ref[:, rows - 1, :].astype(F32)
    for level in range(levels):
        turned = (cell * ocean_ref[level].astype(F32)).T
        turned_ref[level] = turned
        total_ref[level : level + 1, :] = jnp.sum(turned, axis=0, keepdims=True) + small


def weights_of(area, ocean, counted):
    levels, rows, cols = ocean.shape
    return pl.pallas_call(
        weight_kernel,
        in_specs=[pl.BlockSpec(memory_space=VMEM)] * 4,
        out_specs=[pl.BlockSpec(memory_space=VMEM)] * 3,
        out_shape=(
            jax.ShapeDtypeStruct((levels, cols, rows), F32),
            jax.ShapeDtypeStruct((levels, rows), F32),
            jax.ShapeDtypeStruct((levels, cols), F32),
        ),
        compiler_params=params(4),
        name="cell_weights",
    )(first(), area, ocean, counted)


def pick(ref, base, group, offset):
    return ref[pl.ds(base + group * 64 + offset, 8, stride=8), :]


def sums_kernel(fields_ref, turned_ref, part_ref, last_ref, acc_ref, tail_ref):
    count, levels, rows, cols = fields_ref.shape
    per_trip = 4

    def trip(t, carry):
        for k in range(per_trip):
            level = t * per_trip + k
            for f in range(count):
                turned = fields_ref[f, level].T.astype(F32) * turned_ref[level]
                acc = jnp.sum(turned.reshape(cols // 8, 8, rows), axis=0)
                place = pl.multiple_of((f * levels + level) * 8, 8)
                acc_ref[pl.ds(place, 8), :] = acc
                tail_ref[pl.ds(place, 8), :] = fields_ref[f, level, rows - 8 :, :].astype(F32)
        return carry

    lax.fori_loop(0, levels // per_trip, trip, 0)
    for group in range(part_ref.shape[0] // 8):
        total = pick(acc_ref, 0, group, 0)
        for s in range(1, 8):
            total = total + pick(acc_ref, 0, group, s)
        part_ref[group * 8 : group * 8 + 8, :] = total
        last_ref[group * 8 : group * 8 + 8, :] = pick(tail_ref, 0, group, 7)


def row_sums(fields, turned):
    count, levels, rows, cols = fields.shape
    return pl.pallas_call(
        sums_kernel,
        in_specs=[pl.BlockSpec(memory_space=VMEM)] * 2,
        out_specs=[pl.BlockSpec(memory_space=VMEM)] * 2,
        out_shape=(
            jax.ShapeDtypeStruct((count * levels, rows), F32),
            jax.ShapeDtypeStruct((count * levels, cols), F32),
        ),
        scratch_shapes=[
            pltpu.VMEM((count * levels * 8, rows), F32),
            pltpu.VMEM((count * levels * 8, cols), F32),
        ],
        compiler_params=params(16),
        name="row_sums",
    )(fields, turned)


def fold_kernel(part_ref, last_ref, total_ref, cells_ref, partner_ref, counted_ref, keep_ref, send_ref, extra_ref):
    levels, cols = extra_ref.shape
    rows = part_ref.shape[1]
    half = part_ref.shape[0] // 2
    partner = own_columns(partner_ref, cols)
    slot = jnp.bitwise_xor(partner // cols, lax.axis_index("lon"))
    lane = jnp.broadcast_to(partner % cols, (levels, cols))
    extra = jnp.zeros((levels, cols), F32)
    for k in range(cells_ref.shape[0]):
        picked = jnp.take_along_axis(cells_ref[k], lane, axis=1)
        extra = jnp.where(slot == k, picked, extra)
    extra_ref[...] = extra * (0.5 - 0.5 * own_columns(counted_ref, cols).astype(F32))
    fold = jnp.logical_and(lax.broadcasted_iota(jnp.int32, (8, rows), 1) == rows - 1, on_top())
    mine = jnp.bitwise_and(lax.axis_index("lon"), 1)
    for ref, side in ((keep_ref, mine), (send_ref, 1 - mine)):
        for r in range(0, half, 8):
            place = pl.multiple_of(side * half + r, 8)
            part = part_ref[pl.ds(place, 8), :]
            weight = extra_ref[pl.ds(pl.multiple_of(lax.rem(place, levels), 8), 8), :]
            more = jnp.sum(last_ref[pl.ds(place, 8), :] * weight, axis=1, keepdims=True)
            ref[r : r + 8, :] = jnp.where(fold, 0.5 * part + more, part)
    send_ref[half:, :] = total_ref[...]


def add_fold(part, last, total, cells, partner, counted):
    size, rows = part.shape
    levels = total.shape[0]
    return pl.pallas_call(
        fold_kernel,
        in_specs=[pl.BlockSpec(memory_space=VMEM)] * 6,
        out_specs=[pl.BlockSpec(memory_space=VMEM)] * 2,
        out_shape=(
            jax.ShapeDtypeStruct((size // 2, rows), F32),
            jax.ShapeDtypeStruct((size // 2 + levels, rows), F32),
        ),
        scratch_shapes=[pltpu.VMEM((levels, last.shape[1]), F32)],
        compiler_params=params(2),
        name="add_fold",
    )(part, last, total, cells, partner, counted)


def finish_kernel(keep_ref, got_ref, total_ref, code_ref, sum_ref):
    chunk, lanes = keep_ref.shape
    levels = total_ref.shape[0]
    bits = bits_of(lax.axis_size("lon"))
    lon = lax.axis_index("lon")
    start = jnp.int32(0)
    for k in range(len(bits)):
        start = start + jnp.bitwise_and(lon >> k, 1) * (chunk * len_ratio(bits, k))
    sum_ref[...] = total_ref[...] + got_ref[chunk:, :]
    most = jnp.zeros((8, lanes), F32)
    means = []
    for r in range(0, chunk, 8):
        level = pl.multiple_of(lax.rem(start + r, levels), 8)
        part = keep_ref[r : r + 8, :] + got_ref[r : r + 8, :]
        mean = part / sum_ref[pl.ds(level, 8), :]
        most = jnp.maximum(most, jnp.abs(mean))
        means.append(mean)
    most = jnp.maximum(jnp.max(most, axis=0, keepdims=True), TINY)
    power = jnp.minimum(jnp.ceil(jnp.log2(most) * STEPS) + 1.0, 127.0 * STEPS)
    scale = jnp.exp2(power * (1.0 / STEPS))
    for k, mean in enumerate(means):
        code = jnp.clip(jnp.round(mean / scale * TOP), -TOP, TOP)
        code_ref[0, 8 * k : 8 * k + 8, :] = code.astype(jnp.int32).astype(jnp.int16)
    power = jnp.broadcast_to(power, (8, lanes)).astype(jnp.int32)
    code_ref[0, chunk : chunk + 8, :] = power.astype(jnp.int16)


def len_ratio(bits, k):
    return 1 << (len(bits) - 1 - k)


def finish(keep, got, total):
    chunk, lanes = keep.shape
    return pl.pallas_call(
        finish_kernel,
        in_specs=[pl.BlockSpec(memory_space=VMEM)] * 3,
        out_specs=pl.BlockSpec(memory_space=VMEM),
        out_shape=jax.ShapeDtypeStruct((1, chunk + 8, lanes), jnp.int16),
        scratch_shapes=[pltpu.VMEM(total.shape, F32)],
        compiler_params=params(2),
        name="finish",
    )(keep, got, total)


def place_kernel(masks, rows, other, *refs):
    slots_ref, out_ref, mean_ref, sems = refs[0], refs[-3], refs[-2], refs[-1]
    slots, chunk, lanes = mean_ref.shape
    owner_lon = jnp.bitwise_xor(lax.axis_index("lon"), other)
    lon_bits = len(bits_of(lax.axis_size("lon")))
    copies = []
    for s in range(slots):
        power = slots_ref[s, chunk : chunk + 8, :].astype(jnp.int32).astype(F32)
        scale = jnp.exp2(power * (1.0 / STEPS)) * (1.0 / TOP)
        code = slots_ref[s, :chunk, :].astype(jnp.int32).astype(F32)
        mean_ref[s] = (code.reshape(chunk // 8, 8, lanes) * scale[None]).reshape(chunk, lanes)
        dlon, dlat = 0, 0
        for k, mask in enumerate(masks):
            if s >> k & 1:
                dlon, dlat = dlon ^ mask[0], dlat ^ mask[1]
        lon = jnp.bitwise_xor(owner_lon, dlon)
        lat = jnp.bitwise_xor(lax.axis_index("lat"), dlat)
        row = jnp.int32(0)
        for k in range(lon_bits):
            row = row + jnp.bitwise_and(lon >> k, 1) * (rows >> (k + 1))
        dst = out_ref.at[pl.ds(pl.multiple_of(row, 8), chunk), pl.ds(pl.multiple_of(lat * lanes, lanes), lanes)]
        copies.append(pltpu.make_async_copy(mean_ref.at[s], dst, sems.at[s]))
        if s:
            copies[s - 1].start()
    copies[-1].start()
    for copy in copies:
        copy.wait()


def place(slots, into, masks, shape, other):
    args = (slots,) if into is None else (slots, into)
    specs = [pl.BlockSpec(memory_space=VMEM), pl.BlockSpec(memory_space=pl.ANY)]
    count, chunk, lanes = slots.shape
    return pl.pallas_call(
        functools.partial(place_kernel, masks, shape[0], other),
        in_specs=specs[: len(args)],
        out_specs=pl.BlockSpec(memory_space=pl.ANY),
        out_shape=jax.ShapeDtypeStruct(shape, F32),
        scratch_shapes=[
            pltpu.VMEM((count, chunk - 8, lanes), F32),
            pltpu.SemaphoreType.DMA((count,)),
        ],
        input_output_aliases={} if into is None else {1: 0},
        compiler_params=params(4),
        name=f"place_{other}",
    )(*args)


def per_device(fields, area, ocean, partner, counted):
    lon_size, lat_size = lax.axis_size("lon"), lax.axis_size("lat")
    my_lon = lax.axis_index("lon")
    count, levels, lat_rows, lon_cols = fields.shape
    rows = count * levels
    lon_bits = bits_of(lon_size)
    partner, counted = partner[None], counted[None]

    turned, total, cells = weights_of(area, ocean, counted)
    cells = cells[None]
    for bit in lon_bits:
        cells = jnp.concatenate([cells, exchange(cells, "lon", bit)], axis=0)
    part, last = row_sums(fields, turned)
    keep, send = add_fold(part, last, total, cells, partner, counted)

    for bit in lon_bits[1:]:
        half = keep.shape[0]
        got = exchange(send, "lon", bit >> 1)
        part = keep + got[:half]
        total = total + got[half:]
        upper = jnp.bitwise_and(my_lon, bit) != 0
        low, high = part[: half // 2], part[half // 2 :]
        keep = jnp.where(upper, high, low)
        send = jnp.concatenate([jnp.where(upper, low, high), total], axis=0)
    slots = finish(keep, exchange(send, "lon", lon_bits[-1]), total)

    lat_bits = bits_of(lat_size)
    pairs = list(zip(lat_bits, lon_bits[1:]))
    masks = []
    for bit in reversed(lat_bits[len(pairs) :]):
        slots = jnp.concatenate([slots, exchange(slots, "lat", bit)], axis=0)
        masks.append((0, bit))
    for x, y in pairs:
        sent = [exchange(slots, "lat", x), exchange(slots, "lon", y), exchange_both(slots, x, y)]
        slots = jnp.concatenate([slots] + sent, axis=0)
        masks += [(0, x), (y, 0)]
    for bit in lon_bits[1 + len(pairs) :]:
        slots = jnp.concatenate([slots, exchange(slots, "lon", bit)], axis=0)
        masks.append((bit, 0))
    others = exchange(slots, "lon", 1)
    shape = (rows, lat_size * lat_rows)
    out = place(slots, None, masks, shape, 0)
    out = place(others, out, masks, shape, 1)
    return out.reshape(count, levels, lat_size * lat_rows)


def solution(mesh):
    in_specs = (P(None, None, "lat", "lon"), P("lat", "lon"), P(None, "lat", "lon"), P(), P())
    out_specs = P()
    return jax.shard_map(
        per_device, mesh=mesh, in_specs=in_specs, out_specs=out_specs, check_vma=False
    )
```

```python
import functools

import jax
import jax.numpy as jnp
from jax import lax
from jax.experimental import pallas as pl
from jax.experimental.pallas import tpu as pltpu
from jax.sharding import PartitionSpec as P

F32 = jnp.float32
VMEM = pltpu.VMEM
MIB = 1 << 20
TOP = 32767.0
STEPS = 256.0
TINY = 2.0**-126


def params(mib):
    return pltpu.CompilerParams(vmem_limit_bytes=mib * MIB)


def bits_of(size):
    if size & (size - 1):
        raise ValueError("uneven axis")
    return [1 << k for k in range(size.bit_length() - 1)]


def exchange(value, axis, bit):
    size = lax.axis_size(axis)
    return lax.ppermute(value, axis, [(i, i ^ bit) for i in range(size)])


def exchange_both(value, lat_bit, lon_bit):
    lons, lats = lax.axis_size("lon"), lax.axis_size("lat")
    pairs = [(i * lats + j, (i ^ lon_bit) * lats + (j ^ lat_bit)) for i in range(lons) for j in range(lats)]
    return lax.ppermute(value, ("lon", "lat"), pairs)


def own_columns(ref, cols):
    offset = pl.multiple_of(lax.axis_index("lon") * cols, cols)
    return ref[:, pl.ds(offset, cols)]


def on_top():
    return lax.axis_index("lat") == lax.axis_size("lat") - 1


def first_kernel(out_ref):
    out_ref[...] = jnp.zeros_like(out_ref)


def first():
    return pl.pallas_call(
        first_kernel,
        out_specs=pl.BlockSpec(memory_space=VMEM),
        out_shape=jax.ShapeDtypeStruct((8, 128), F32),
        compiler_params=params(1),
        cost_estimate=pl.CostEstimate(flops=4_000_000_000, bytes_accessed=100, transcendentals=0),
        name="first",
    )()


def weight_kernel(_, area_ref, ocean_ref, counted_ref, turned_ref, shared_ref):
    levels, rows, cols = ocean_ref.shape
    counted = own_columns(counted_ref, cols).astype(F32)
    row = lax.broadcasted_iota(jnp.int32, (rows, cols), 0)
    fold = jnp.logical_and(row == rows - 1, on_top())
    cell = jnp.where(fold, counted, F32(1.0)) * area_ref[...]
    small = 0.05 * jnp.sum(cell.T, axis=0, keepdims=True)
    shared_ref[:levels, :] = area_ref[rows - 1 :, :] * ocean_ref[:, rows - 1, :].astype(F32)
    for level in range(levels):
        turned = (cell * ocean_ref[level].astype(F32)).T
        turned_ref[level] = turned
        place = levels + level
        shared_ref[place : place + 1, :] = jnp.sum(turned, axis=0, keepdims=True) + small


def weights_of(area, ocean, counted):
    levels, rows, cols = ocean.shape
    assert rows == cols
    return pl.pallas_call(
        weight_kernel,
        in_specs=[pl.BlockSpec(memory_space=VMEM)] * 4,
        out_specs=[pl.BlockSpec(memory_space=VMEM)] * 2,
        out_shape=(
            jax.ShapeDtypeStruct((levels, cols, rows), F32),
            jax.ShapeDtypeStruct((2 * levels, cols), F32),
        ),
        compiler_params=params(4),
        name="cell_weights",
    )(first(), area, ocean, counted)


def pick(ref, base, group, offset):
    return ref[pl.ds(base + group * 64 + offset, 8, stride=8), :]


def sums_kernel(fields_ref, turned_ref, part_ref, last_ref, acc_ref, tail_ref):
    count, levels, rows, cols = fields_ref.shape
    per_trip = 4

    def trip(t, carry):
        for k in range(per_trip):
            level = t * per_trip + k
            for f in range(count):
                turned = fields_ref[f, level].T.astype(F32) * turned_ref[level]
                acc = jnp.sum(turned.reshape(cols // 8, 8, rows), axis=0)
                place = pl.multiple_of((f * levels + level) * 8, 8)
                acc_ref[pl.ds(place, 8), :] = acc
                tail_ref[pl.ds(place, 8), :] = fields_ref[f, level, rows - 8 :, :].astype(F32)
        return carry

    lax.fori_loop(0, levels // per_trip, trip, 0)
    for group in range(part_ref.shape[0] // 8):
        total = pick(acc_ref, 0, group, 0)
        for s in range(1, 8):
            total = total + pick(acc_ref, 0, group, s)
        part_ref[group * 8 : group * 8 + 8, :] = total
        last_ref[group * 8 : group * 8 + 8, :] = pick(tail_ref, 0, group, 7)


def row_sums(fields, turned):
    count, levels, rows, cols = fields.shape
    return pl.pallas_call(
        sums_kernel,
        in_specs=[pl.BlockSpec(memory_space=VMEM)] * 2,
        out_specs=[pl.BlockSpec(memory_space=VMEM)] * 2,
        out_shape=(
            jax.ShapeDtypeStruct((count * levels, rows), F32),
            jax.ShapeDtypeStruct((count * levels, cols), F32),
        ),
        scratch_shapes=[
            pltpu.VMEM((count * levels * 8, rows), F32),
            pltpu.VMEM((count * levels * 8, cols), F32),
        ],
        compiler_params=params(16),
        name="row_sums",
    )(fields, turned)


def chunk_start(lon, chunk, size):
    start = jnp.int32(0)
    for k in range(len(bits_of(size))):
        start = start + jnp.bitwise_and(lon >> k, 1) * (chunk * (size >> (k + 1)))
    return pl.multiple_of(start, 8)


def fold_kernel(part_ref, last_ref, shared_ref, partner_ref, counted_ref, *refs):
    piece_refs, extra_ref = refs[:-1], refs[-1]
    levels, cols = extra_ref.shape
    chunk, rows = piece_refs[0].shape
    partner = own_columns(partner_ref, cols)
    slot = jnp.bitwise_xor(partner // cols, lax.axis_index("lon"))
    lane = jnp.broadcast_to(partner % cols, (levels, cols))
    extra = jnp.zeros((levels, cols), F32)
    for k in range(shared_ref.shape[0]):
        picked = jnp.take_along_axis(shared_ref[k, :levels, :], lane, axis=1)
        extra = jnp.where(slot == k, picked, extra)
    extra_ref[...] = extra * (0.5 - 0.5 * own_columns(counted_ref, cols).astype(F32))
    fold = jnp.logical_and(lax.broadcasted_iota(jnp.int32, (8, rows), 1) == rows - 1, on_top())
    for mask, ref in enumerate(piece_refs):
        start = chunk_start(jnp.bitwise_xor(lax.axis_index("lon"), mask), chunk, len(piece_refs))
        for r in range(0, chunk, 8):
            place = pl.multiple_of(start + r, 8)
            part = part_ref[pl.ds(place, 8), :]
            weight = extra_ref[pl.ds(pl.multiple_of(lax.rem(place, levels), 8), 8), :]
            more = jnp.sum(last_ref[pl.ds(place, 8), :] * weight, axis=1, keepdims=True)
            ref[r : r + 8, :] = jnp.where(fold, 0.5 * part + more, part)


def add_fold(part, last, shared, partner, counted):
    size, rows = part.shape
    members, levels = shared.shape[0], shared.shape[1] // 2
    chunk = size // members
    return pl.pallas_call(
        fold_kernel,
        in_specs=[pl.BlockSpec(memory_space=VMEM)] * 5,
        out_specs=[pl.BlockSpec(memory_space=VMEM)] * members,
        out_shape=[jax.ShapeDtypeStruct((chunk, rows), F32)] * members,
        scratch_shapes=[pltpu.VMEM((levels, last.shape[1]), F32)],
        compiler_params=params(2),
        name="add_fold",
    )(part, last, shared, partner, counted)


def finish_kernel(shared_ref, *refs):
    part_refs, code_ref, sum_ref = refs[:-2], refs[-2], refs[-1]
    chunk, lanes = part_refs[0].shape
    levels = sum_ref.shape[0]
    start = chunk_start(lax.axis_index("lon"), chunk, len(part_refs))
    total = shared_ref[0, levels:, :]
    for k in range(1, shared_ref.shape[0]):
        total = total + shared_ref[k, levels:, :]
    sum_ref[...] = total
    most = jnp.zeros((8, lanes), F32)
    means = []
    for r in range(0, chunk, 8):
        level = pl.multiple_of(lax.rem(start + r, levels), 8)
        part = part_refs[0][r : r + 8, :]
        for ref in part_refs[1:]:
            part = part + ref[r : r + 8, :]
        mean = part / sum_ref[pl.ds(level, 8), :]
        most = jnp.maximum(most, jnp.abs(mean))
        means.append(mean)
    most = jnp.maximum(jnp.max(most, axis=0, keepdims=True), TINY)
    power = jnp.minimum(jnp.ceil(jnp.log2(most) * STEPS) + 1.0, 127.0 * STEPS)
    scale = jnp.exp2(power * (1.0 / STEPS))
    for k, mean in enumerate(means):
        code = jnp.clip(jnp.round(mean / scale * TOP), -TOP, TOP)
        code_ref[0, 8 * k : 8 * k + 8, :] = code.astype(jnp.int32).astype(jnp.int16)
    power = jnp.broadcast_to(power, (8, lanes)).astype(jnp.int32)
    code_ref[0, chunk : chunk + 8, :] = power.astype(jnp.int16)


def finish(shared, parts):
    chunk, lanes = parts[0].shape
    return pl.pallas_call(
        finish_kernel,
        in_specs=[pl.BlockSpec(memory_space=VMEM)] * (1 + len(parts)),
        out_specs=pl.BlockSpec(memory_space=VMEM),
        out_shape=jax.ShapeDtypeStruct((1, chunk + 8, lanes), jnp.int16),
        scratch_shapes=[pltpu.VMEM((shared.shape[1] // 2, lanes), F32)],
        compiler_params=params(2),
        name="finish",
    )(shared, *parts)


def place_kernel(masks, other, *refs):
    slots_ref, out_ref, mean_ref, sems = refs[0], refs[-3], refs[-2], refs[-1]
    slots, chunk, lanes = mean_ref.shape
    owner_lon = jnp.bitwise_xor(lax.axis_index("lon"), other)
    copies = []
    for s in range(slots):
        power = slots_ref[s, chunk : chunk + 8, :].astype(jnp.int32).astype(F32)
        scale = jnp.exp2(power * (1.0 / STEPS)) * (1.0 / TOP)
        code = slots_ref[s, :chunk, :].astype(jnp.int32).astype(F32)
        mean_ref[s] = (code.reshape(chunk // 8, 8, lanes) * scale[None]).reshape(chunk, lanes)
        dlon, dlat = 0, 0
        for k, mask in enumerate(masks):
            if s >> k & 1:
                dlon, dlat = dlon ^ mask[0], dlat ^ mask[1]
        lon = jnp.bitwise_xor(owner_lon, dlon)
        lat = jnp.bitwise_xor(lax.axis_index("lat"), dlat)
        row = chunk_start(lon, chunk, lax.axis_size("lon"))
        dst = out_ref.at[pl.ds(row, chunk), pl.ds(pl.multiple_of(lat * lanes, lanes), lanes)]
        copies.append(pltpu.make_async_copy(mean_ref.at[s], dst, sems.at[s]))
        if s:
            copies[s - 1].start()
    copies[-1].start()
    for copy in copies:
        copy.wait()


def place(slots, into, masks, shape, other):
    args = (slots,) if into is None else (slots, into)
    specs = [pl.BlockSpec(memory_space=VMEM), pl.BlockSpec(memory_space=pl.ANY)]
    count, chunk, lanes = slots.shape
    return pl.pallas_call(
        functools.partial(place_kernel, masks, other),
        in_specs=specs[: len(args)],
        out_specs=pl.BlockSpec(memory_space=pl.ANY),
        out_shape=jax.ShapeDtypeStruct(shape, F32),
        scratch_shapes=[
            pltpu.VMEM((count, chunk - 8, lanes), F32),
            pltpu.SemaphoreType.DMA((count,)),
        ],
        input_output_aliases={} if into is None else {1: 0},
        compiler_params=params(4),
        name=f"place_{other}",
    )(*args)


def per_device(fields, area, ocean, partner, counted):
    lon_size, lat_size = lax.axis_size("lon"), lax.axis_size("lat")
    count, levels, lat_rows, lon_cols = fields.shape
    rows = count * levels
    lon_bits = bits_of(lon_size)
    partner, counted = partner[None], counted[None]

    turned, shared = weights_of(area, ocean, counted)
    shared = shared[None]
    for bit in lon_bits:
        shared = jnp.concatenate([shared, exchange(shared, "lon", bit)], axis=0)
    part, last = row_sums(fields, turned)
    pieces = add_fold(part, last, shared, partner, counted)

    got = [exchange(pieces[mask], "lon", mask) for mask in range(1, lon_size)]
    slots = finish(shared, [pieces[0]] + got)

    lat_bits = bits_of(lat_size)
    pairs = list(zip(lat_bits, lon_bits[1:]))
    masks = []
    for bit in reversed(lat_bits[len(pairs) :]):
        slots = jnp.concatenate([slots, exchange(slots, "lat", bit)], axis=0)
        masks.append((0, bit))
    for x, y in pairs:
        sent = [exchange(slots, "lat", x), exchange(slots, "lon", y), exchange_both(slots, x, y)]
        slots = jnp.concatenate([slots] + sent, axis=0)
        masks += [(0, x), (y, 0)]
    for bit in lon_bits[1 + len(pairs) :]:
        slots = jnp.concatenate([slots, exchange(slots, "lon", bit)], axis=0)
        masks.append((bit, 0))
    others = exchange(slots, "lon", 1)
    shape = (rows, lat_size * lat_rows)
    out = place(slots, None, masks, shape, 0)
    out = place(others, out, masks, shape, 1)
    return out.reshape(count, levels, lat_size * lat_rows)


def solution(mesh):
    in_specs = (P(None, None, "lat", "lon"), P("lat", "lon"), P(None, "lat", "lon"), P(), P())
    out_specs = P()
    return jax.shard_map(
        per_device, mesh=mesh, in_specs=in_specs, out_specs=out_specs, check_vma=False
    )
```

```python
import functools

import jax
import jax.numpy as jnp
from jax import lax
from jax.experimental import pallas as pl
from jax.experimental.pallas import tpu as pltpu
from jax.sharding import PartitionSpec as P


F32 = jnp.float32
VMEM = pltpu.VMEM
MIB = 1 << 20
TOP = 32767.0
STEPS = 256.0
TINY = 2.0**-126


def params(mib):
    return pltpu.CompilerParams(vmem_limit_bytes=mib * MIB)


def bits_of(size):
    if size & (size - 1):
        raise ValueError("uneven axis")
    return [1 << k for k in range(size.bit_length() - 1)]


def paired_bits(lon_size, lat_size):
    return list(zip(bits_of(lat_size), bits_of(lon_size)[1:]))


def exchange(value, axis, bit):
    size = lax.axis_size(axis)
    return lax.ppermute(value, axis, [(i, i ^ bit) for i in range(size)])


def exchange_both(value, lat_bit, lon_bit):
    lons, lats = lax.axis_size("lon"), lax.axis_size("lat")
    pairs = [(i * lats + j, (i ^ lon_bit) * lats + (j ^ lat_bit)) for i in range(lons) for j in range(lats)]
    return lax.ppermute(value, ("lon", "lat"), pairs)


def own_columns(ref, cols):
    offset = pl.multiple_of(lax.axis_index("lon") * cols, cols)
    return ref[:, pl.ds(offset, cols)]


def on_top():
    return lax.axis_index("lat") == lax.axis_size("lat") - 1


def first_kernel(out_ref):
    out_ref[...] = jnp.zeros_like(out_ref)


def first():
    return pl.pallas_call(
        first_kernel,
        out_specs=pl.BlockSpec(memory_space=VMEM),
        out_shape=jax.ShapeDtypeStruct((8, 128), F32),
        compiler_params=params(1),
        cost_estimate=pl.CostEstimate(flops=4_000_000_000, bytes_accessed=100, transcendentals=0),
        name="first",
    )()


def weight_kernel(_, area_ref, ocean_ref, counted_ref, turned_ref, shared_ref):
    levels, rows, cols = ocean_ref.shape
    counted = own_columns(counted_ref, cols).astype(F32)
    row = lax.broadcasted_iota(jnp.int32, (rows, cols), 0)
    fold = jnp.logical_and(row == rows - 1, on_top())
    cell = jnp.where(fold, counted, F32(1.0)) * area_ref[...]
    small = 0.05 * jnp.sum(cell.T, axis=0, keepdims=True)
    shared_ref[:levels, :] = area_ref[rows - 1 :, :] * ocean_ref[:, rows - 1, :].astype(F32)
    for level in range(levels):
        turned = (cell * ocean_ref[level].astype(F32)).T
        turned_ref[level] = turned
        place = levels + level
        shared_ref[place : place + 1, :] = jnp.sum(turned, axis=0, keepdims=True) + small


def weights_of(area, ocean, counted):
    levels, rows, cols = ocean.shape
    assert rows == cols
    return pl.pallas_call(
        weight_kernel,
        in_specs=[pl.BlockSpec(memory_space=VMEM)] * 4,
        out_specs=[pl.BlockSpec(memory_space=VMEM)] * 2,
        out_shape=(
            jax.ShapeDtypeStruct((levels, cols, rows), F32),
            jax.ShapeDtypeStruct((2 * levels, cols), F32),
        ),
        compiler_params=params(4),
        name="cell_weights",
    )(first(), area, ocean, counted)


def pick(ref, base, group, offset):
    return ref[pl.ds(base + group * 64 + offset, 8, stride=8), :]


def sums_kernel(fields_ref, turned_ref, part_ref, last_ref, acc_ref, tail_ref):
    count, levels, rows, cols = fields_ref.shape
    per_trip = 16

    def trip(t, carry):
        for k in range(per_trip):
            level = t * per_trip + k
            for f in range(count):
                turned = fields_ref[f, level].T.astype(F32) * turned_ref[level]
                acc = jnp.sum(turned.reshape(cols // 8, 8, rows), axis=0)
                place = pl.multiple_of((f * levels + level) * 8, 8)
                acc_ref[pl.ds(place, 8), :] = acc
                tail_ref[pl.ds(place, 8), :] = fields_ref[f, level, rows - 8 :, :].astype(F32)
        return carry

    lax.fori_loop(0, levels // per_trip, trip, 0)
    for group in range(part_ref.shape[0] // 8):
        total = pick(acc_ref, 0, group, 0)
        for s in range(1, 8):
            total = total + pick(acc_ref, 0, group, s)
        part_ref[group * 8 : group * 8 + 8, :] = total
        last_ref[group * 8 : group * 8 + 8, :] = pick(tail_ref, 0, group, 7)


def row_sums(fields, turned):
    count, levels, rows, cols = fields.shape
    return pl.pallas_call(
        sums_kernel,
        in_specs=[pl.BlockSpec(memory_space=VMEM)] * 2,
        out_specs=[pl.BlockSpec(memory_space=VMEM)] * 2,
        out_shape=(
            jax.ShapeDtypeStruct((count * levels, rows), F32),
            jax.ShapeDtypeStruct((count * levels, cols), F32),
        ),
        scratch_shapes=[
            pltpu.VMEM((count * levels * 8, rows), F32),
            pltpu.VMEM((count * levels * 8, cols), F32),
        ],
        compiler_params=params(16),
        name="row_sums",
    )(fields, turned)


def chunk_start(lon, chunk, size):
    start = jnp.int32(0)
    for k in range(len(bits_of(size))):
        start = start + jnp.bitwise_and(lon >> k, 1) * (chunk * (size >> (k + 1)))
    return pl.multiple_of(start, 8)


def fold_kernel(part_ref, last_ref, shared_ref, partner_ref, counted_ref, *refs):
    piece_refs, extra_ref = refs[:-1], refs[-1]
    levels, cols = extra_ref.shape
    chunk, rows = piece_refs[0].shape
    partner = own_columns(partner_ref, cols)
    slot = jnp.bitwise_xor(partner // cols, lax.axis_index("lon"))
    lane = jnp.broadcast_to(partner % cols, (levels, cols))
    extra = jnp.zeros((levels, cols), F32)
    for k in range(shared_ref.shape[0]):
        picked = jnp.take_along_axis(shared_ref[k, :levels, :], lane, axis=1)
        extra = jnp.where(slot == k, picked, extra)
    extra_ref[...] = extra * (0.5 - 0.5 * own_columns(counted_ref, cols).astype(F32))
    fold = jnp.logical_and(lax.broadcasted_iota(jnp.int32, (8, rows), 1) == rows - 1, on_top())
    for mask, ref in enumerate(piece_refs):
        start = chunk_start(jnp.bitwise_xor(lax.axis_index("lon"), mask), chunk, len(piece_refs))
        for r in range(0, chunk, 8):
            place = pl.multiple_of(start + r, 8)
            part = part_ref[pl.ds(place, 8), :]
            weight = extra_ref[pl.ds(pl.multiple_of(lax.rem(place, levels), 8), 8), :]
            more = jnp.sum(last_ref[pl.ds(place, 8), :] * weight, axis=1, keepdims=True)
            ref[r : r + 8, :] = jnp.where(fold, 0.5 * part + more, part)


def add_fold(part, last, shared, partner, counted):
    size, rows = part.shape
    members, levels = shared.shape[0], shared.shape[1] // 2
    chunk = size // members
    return pl.pallas_call(
        fold_kernel,
        in_specs=[pl.BlockSpec(memory_space=VMEM)] * 5,
        out_specs=[pl.BlockSpec(memory_space=VMEM)] * members,
        out_shape=[jax.ShapeDtypeStruct((chunk, rows), F32)] * members,
        scratch_shapes=[pltpu.VMEM((levels, last.shape[1]), F32)],
        compiler_params=params(2),
        name="add_fold",
    )(part, last, shared, partner, counted)


def finish_kernel(shared_ref, *refs):
    part_refs, code_ref, sum_ref = refs[:-2], refs[-2], refs[-1]
    chunk, lanes = part_refs[0].shape
    levels = sum_ref.shape[0]
    start = chunk_start(lax.axis_index("lon"), chunk, len(part_refs))
    total = shared_ref[0, levels:, :]
    for k in range(1, shared_ref.shape[0]):
        total = total + shared_ref[k, levels:, :]
    sum_ref[...] = total
    most = jnp.zeros((8, lanes), F32)
    means = []
    for r in range(0, chunk, 8):
        level = pl.multiple_of(lax.rem(start + r, levels), 8)
        part = part_refs[0][r : r + 8, :]
        for ref in part_refs[1:]:
            part = part + ref[r : r + 8, :]
        mean = part / sum_ref[pl.ds(level, 8), :]
        most = jnp.maximum(most, jnp.abs(mean))
        means.append(mean)
    most = jnp.maximum(jnp.max(most, axis=0, keepdims=True), TINY)
    power = jnp.minimum(jnp.ceil(jnp.log2(most) * STEPS) + 1.0, 127.0 * STEPS)
    scale = jnp.exp2(power * (1.0 / STEPS))
    for k, mean in enumerate(means):
        code = jnp.clip(jnp.round(mean / scale * TOP), -TOP, TOP)
        code_ref[0, 8 * k : 8 * k + 8, :] = code.astype(jnp.int32).astype(jnp.int16)
    power = jnp.broadcast_to(power, (8, lanes)).astype(jnp.int32)
    code_ref[0, chunk : chunk + 8, :] = power.astype(jnp.int16)


def finish(shared, parts):
    chunk, lanes = parts[0].shape
    return pl.pallas_call(
        finish_kernel,
        in_specs=[pl.BlockSpec(memory_space=VMEM)] * (1 + len(parts)),
        out_specs=pl.BlockSpec(memory_space=VMEM),
        out_shape=jax.ShapeDtypeStruct((1, chunk + 8, lanes), jnp.int16),
        scratch_shapes=[pltpu.VMEM((shared.shape[1] // 2, lanes), F32)],
        compiler_params=params(2),
        name="finish",
    )(shared, *parts)


def place_kernel(masks, other, *refs):
    slots_ref, out_ref, mean_ref, sems = refs[0], refs[-3], refs[-2], refs[-1]
    slots, chunk, lanes = mean_ref.shape
    owner_lon = jnp.bitwise_xor(lax.axis_index("lon"), other)
    copies = []
    for s in range(slots):
        power = slots_ref[s, chunk : chunk + 8, :].astype(jnp.int32).astype(F32)
        scale = jnp.exp2(power * (1.0 / STEPS)) * (1.0 / TOP)
        code = slots_ref[s, :chunk, :].astype(jnp.int32).astype(F32)
        mean_ref[s] = (code.reshape(chunk // 8, 8, lanes) * scale[None]).reshape(chunk, lanes)
        dlon, dlat = 0, 0
        for k, mask in enumerate(masks):
            if s >> k & 1:
                dlon, dlat = dlon ^ mask[0], dlat ^ mask[1]
        lon = jnp.bitwise_xor(owner_lon, dlon)
        lat = jnp.bitwise_xor(lax.axis_index("lat"), dlat)
        row = chunk_start(lon, chunk, lax.axis_size("lon"))
        dst = out_ref.at[pl.ds(row, chunk), pl.ds(pl.multiple_of(lat * lanes, lanes), lanes)]
        copies.append(pltpu.make_async_copy(mean_ref.at[s], dst, sems.at[s]))
        if s:
            copies[s - 1].start()
    copies[-1].start()
    for copy in copies:
        copy.wait()


def place(slots, into, masks, shape, other):
    args = (slots,) if into is None else (slots, into)
    specs = [pl.BlockSpec(memory_space=VMEM), pl.BlockSpec(memory_space=pl.ANY)]
    count, chunk, lanes = slots.shape
    return pl.pallas_call(
        functools.partial(place_kernel, masks, other),
        in_specs=specs[: len(args)],
        out_specs=pl.BlockSpec(memory_space=pl.ANY),
        out_shape=jax.ShapeDtypeStruct(shape, F32),
        scratch_shapes=[
            pltpu.VMEM((count, chunk - 8, lanes), F32),
            pltpu.SemaphoreType.DMA((count,)),
        ],
        input_output_aliases={} if into is None else {1: 0},
        compiler_params=params(4),
    )(*args)


def zonal_means(fields, area, ocean, partner, counted):
    lon_size, lat_size = lax.axis_size("lon"), lax.axis_size("lat")
    count, levels, lat_rows, _ = fields.shape
    rows = count * levels
    lon_bits = bits_of(lon_size)
    partner, counted = partner[None], counted[None]

    turned, shared = weights_of(area, ocean, counted)
    shared = shared[None]
    for bit in lon_bits:
        shared = jnp.concatenate([shared, exchange(shared, "lon", bit)], axis=0)
    part, last = row_sums(fields, turned)
    pieces = add_fold(part, last, shared, partner, counted)

    got = []
    for mask in range(1, lon_size):
        got.append(exchange(pieces[mask], "lon", mask))
    slots = finish(shared, [pieces[0]] + got)

    lat_bits = bits_of(lat_size)
    pairs = paired_bits(lon_size, lat_size)
    masks = []
    for bit in reversed(lat_bits[len(pairs) :]):
        slots = jnp.concatenate([slots, exchange(slots, "lat", bit)], axis=0)
        masks.append((0, bit))
    for x, y in pairs:
        sent = [exchange(slots, "lat", x)]
        sent.append(exchange(slots, "lon", y))
        sent.append(exchange_both(slots, x, y))
        slots = jnp.concatenate([slots] + sent, axis=0)
        masks += [(0, x), (y, 0)]
    for bit in lon_bits[1 + len(pairs) :]:
        slots = jnp.concatenate([slots, exchange(slots, "lon", bit)], axis=0)
        masks.append((bit, 0))
    others = exchange(slots, "lon", 1)
    shape = (rows, lat_size * lat_rows)
    out = place(slots, None, masks, shape, 0)
    out = place(others, out, masks, shape, 1)
    return out.reshape(count, levels, lat_size * lat_rows)


def solution(mesh):
    in_specs = (P(None, None, "lat", "lon"), P("lat", "lon"), P(None, "lat", "lon"), P(), P())
    return jax.shard_map(zonal_means, mesh=mesh, in_specs=in_specs, out_specs=P(), check_vma=False)
```

```python
import functools

import jax
import jax.numpy as jnp
from jax import lax
from jax.experimental import pallas as pl
from jax.experimental.pallas import tpu as pltpu
from jax.sharding import PartitionSpec as P


F32 = jnp.float32
VMEM = pltpu.VMEM
MIB = 1 << 20
TOP = 32767.0
STEPS = 256.0
TINY = 2.0**-126


def params(mib):
    return pltpu.CompilerParams(vmem_limit_bytes=mib * MIB)


def bits_of(size):
    if size & (size - 1):
        raise ValueError("uneven axis")
    return [1 << k for k in range(size.bit_length() - 1)]


def rounds_of(lon_size, lat_size):
    lat_bits, y_bits = bits_of(lat_size), bits_of(lon_size)[1:]
    z_bits = lat_bits[len(y_bits) :]
    z_steps = [(0, bit, bit // z_bits[0]) for bit in z_bits]
    rounds = [z_steps[k : k + 2] for k in range(0, len(z_steps), 2)]
    rounds += [[(0, x, x), (y, 0, y // 2)] for x, y in zip(lat_bits, y_bits)]
    return rounds + [[(y, 0, y // 2)] for y in y_bits[len(lat_bits) :]]


def exchange(value, axis, bit):
    size = lax.axis_size(axis)
    return lax.ppermute(value, axis, [(i, i ^ bit) for i in range(size)])


def exchange_both(value, lat_bit, lon_bit):
    lons, lats = lax.axis_size("lon"), lax.axis_size("lat")
    pairs = [(i * lats + j, (i ^ lon_bit) * lats + (j ^ lat_bit)) for i in range(lons) for j in range(lats)]
    return lax.ppermute(value, ("lon", "lat"), pairs)


def own_columns(ref, cols):
    offset = pl.multiple_of(lax.axis_index("lon") * cols, cols)
    return ref[:, pl.ds(offset, cols)]


def on_top():
    return lax.axis_index("lat") == lax.axis_size("lat") - 1


def first_kernel(out_ref):
    out_ref[...] = jnp.zeros_like(out_ref)


def first():
    return pl.pallas_call(
        first_kernel,
        out_specs=pl.BlockSpec(memory_space=VMEM),
        out_shape=jax.ShapeDtypeStruct((8, 128), F32),
        compiler_params=params(1),
        cost_estimate=pl.CostEstimate(flops=4_000_000_000, bytes_accessed=100, transcendentals=0),
        name="first",
    )()


def weight_kernel(_, area_ref, ocean_ref, counted_ref, turned_ref, shared_ref):
    levels, rows, cols = ocean_ref.shape
    counted = own_columns(counted_ref, cols).astype(F32)
    row = lax.broadcasted_iota(jnp.int32, (rows, cols), 0)
    fold = jnp.logical_and(row == rows - 1, on_top())
    cell = jnp.where(fold, counted, F32(1.0)) * area_ref[...]
    small = 0.05 * jnp.sum(cell.T, axis=0, keepdims=True)
    shared_ref[:levels, :] = area_ref[rows - 1 :, :] * ocean_ref[:, rows - 1, :].astype(F32)
    for level in range(levels):
        turned = (cell * ocean_ref[level].astype(F32)).T
        turned_ref[level] = turned
        place = levels + level
        shared_ref[place : place + 1, :] = jnp.sum(turned, axis=0, keepdims=True) + small


def weights_of(area, ocean, counted):
    levels, rows, cols = ocean.shape
    assert rows == cols
    return pl.pallas_call(
        weight_kernel,
        in_specs=[pl.BlockSpec(memory_space=VMEM)] * 4,
        out_specs=[pl.BlockSpec(memory_space=VMEM)] * 2,
        out_shape=(
            jax.ShapeDtypeStruct((levels, cols, rows), F32),
            jax.ShapeDtypeStruct((2 * levels, cols), F32),
        ),
        compiler_params=params(4),
        name="cell_weights",
    )(first(), area, ocean, counted)


def pick(ref, base, group, offset):
    return ref[pl.ds(base + group * 64 + offset, 8, stride=8), :]


def sums_kernel(fields_ref, turned_ref, part_ref, last_ref, acc_ref, tail_ref):
    count, levels, rows, cols = fields_ref.shape
    per_trip = 16

    def trip(t, carry):
        for k in range(per_trip):
            level = t * per_trip + k
            for f in range(count):
                turned = fields_ref[f, level].T.astype(F32) * turned_ref[level]
                acc = jnp.sum(turned.reshape(cols // 8, 8, rows), axis=0)
                place = pl.multiple_of((f * levels + level) * 8, 8)
                acc_ref[pl.ds(place, 8), :] = acc
                tail_ref[pl.ds(place, 8), :] = fields_ref[f, level, rows - 8 :, :].astype(F32)
        return carry

    lax.fori_loop(0, levels // per_trip, trip, 0)
    for group in range(part_ref.shape[0] // 8):
        total = pick(acc_ref, 0, group, 0)
        for s in range(1, 8):
            total = total + pick(acc_ref, 0, group, s)
        part_ref[group * 8 : group * 8 + 8, :] = total
        last_ref[group * 8 : group * 8 + 8, :] = pick(tail_ref, 0, group, 7)


def row_sums(fields, turned):
    count, levels, rows, cols = fields.shape
    return pl.pallas_call(
        sums_kernel,
        in_specs=[pl.BlockSpec(memory_space=VMEM)] * 2,
        out_specs=[pl.BlockSpec(memory_space=VMEM)] * 2,
        out_shape=(
            jax.ShapeDtypeStruct((count * levels, rows), F32),
            jax.ShapeDtypeStruct((count * levels, cols), F32),
        ),
        scratch_shapes=[
            pltpu.VMEM((count * levels * 8, rows), F32),
            pltpu.VMEM((count * levels * 8, cols), F32),
        ],
        compiler_params=params(16),
        name="row_sums",
    )(fields, turned)


def chunk_start(lon, chunk, size):
    start = jnp.int32(0)
    for k in range(len(bits_of(size))):
        start = start + jnp.bitwise_and(lon >> k, 1) * (chunk * (size >> (k + 1)))
    return pl.multiple_of(start, 8)


def fold_kernel(part_ref, last_ref, shared_ref, partner_ref, counted_ref, *refs):
    piece_refs, extra_ref = refs[:-1], refs[-1]
    levels, cols = extra_ref.shape
    chunk, rows = piece_refs[0].shape
    partner = own_columns(partner_ref, cols)
    slot = jnp.bitwise_xor(partner // cols, lax.axis_index("lon"))
    lane = jnp.broadcast_to(partner % cols, (levels, cols))
    extra = jnp.zeros((levels, cols), F32)
    for k in range(shared_ref.shape[0]):
        picked = jnp.take_along_axis(shared_ref[k, :levels, :], lane, axis=1)
        extra = jnp.where(slot == k, picked, extra)
    extra_ref[...] = extra * (0.5 - 0.5 * own_columns(counted_ref, cols).astype(F32))
    fold = jnp.logical_and(lax.broadcasted_iota(jnp.int32, (8, rows), 1) == rows - 1, on_top())
    for mask, ref in enumerate(piece_refs):
        start = chunk_start(jnp.bitwise_xor(lax.axis_index("lon"), mask), chunk, len(piece_refs))
        for r in range(0, chunk, 8):
            place = pl.multiple_of(start + r, 8)
            part = part_ref[pl.ds(place, 8), :]
            weight = extra_ref[pl.ds(pl.multiple_of(lax.rem(place, levels), 8), 8), :]
            more = jnp.sum(last_ref[pl.ds(place, 8), :] * weight, axis=1, keepdims=True)
            ref[r : r + 8, :] = jnp.where(fold, 0.5 * part + more, part)


def add_fold(part, last, shared, partner, counted):
    size, rows = part.shape
    members, levels = shared.shape[0], shared.shape[1] // 2
    chunk = size // members
    return pl.pallas_call(
        fold_kernel,
        in_specs=[pl.BlockSpec(memory_space=VMEM)] * 5,
        out_specs=[pl.BlockSpec(memory_space=VMEM)] * members,
        out_shape=[jax.ShapeDtypeStruct((chunk, rows), F32)] * members,
        scratch_shapes=[pltpu.VMEM((levels, last.shape[1]), F32)],
        compiler_params=params(2),
        name="add_fold",
    )(part, last, shared, partner, counted)


def finish_kernel(shared_ref, *refs):
    part_refs, code_ref, sum_ref = refs[:-2], refs[-2], refs[-1]
    chunk, lanes = part_refs[0].shape
    levels = sum_ref.shape[0]
    start = chunk_start(lax.axis_index("lon"), chunk, len(part_refs))
    total = shared_ref[0, levels:, :]
    for k in range(1, shared_ref.shape[0]):
        total = total + shared_ref[k, levels:, :]
    sum_ref[...] = total
    most = jnp.zeros((8, lanes), F32)
    means = []
    for r in range(0, chunk, 8):
        level = pl.multiple_of(lax.rem(start + r, levels), 8)
        part = part_refs[0][r : r + 8, :]
        for ref in part_refs[1:]:
            part = part + ref[r : r + 8, :]
        mean = part / sum_ref[pl.ds(level, 8), :]
        most = jnp.maximum(most, jnp.abs(mean))
        means.append(mean)
    most = jnp.maximum(jnp.max(most, axis=0, keepdims=True), TINY)
    power = jnp.minimum(jnp.ceil(jnp.log2(most) * STEPS) + 1.0, 127.0 * STEPS)
    scale = jnp.exp2(power * (1.0 / STEPS))
    for k, mean in enumerate(means):
        code = jnp.clip(jnp.round(mean / scale * TOP), -TOP, TOP)
        code_ref[0, 8 * k : 8 * k + 8, :] = code.astype(jnp.int32).astype(jnp.int16)
    power = jnp.broadcast_to(power, (8, lanes)).astype(jnp.int32)
    code_ref[0, chunk : chunk + 8, :] = power.astype(jnp.int16)


def finish(shared, parts):
    chunk, lanes = parts[0].shape
    return pl.pallas_call(
        finish_kernel,
        in_specs=[pl.BlockSpec(memory_space=VMEM)] * (1 + len(parts)),
        out_specs=pl.BlockSpec(memory_space=VMEM),
        out_shape=jax.ShapeDtypeStruct((1, chunk + 8, lanes), jnp.int16),
        scratch_shapes=[pltpu.VMEM((shared.shape[1] // 2, lanes), F32)],
        compiler_params=params(2),
        name="finish",
    )(shared, *parts)


def place_kernel(masks, other, *refs):
    slots_ref, out_ref, mean_ref, sems = refs[0], refs[-3], refs[-2], refs[-1]
    slots, chunk, lanes = mean_ref.shape
    owner_lon = jnp.bitwise_xor(lax.axis_index("lon"), other)
    copies = []
    for s in range(slots):
        power = slots_ref[s, chunk : chunk + 8, :].astype(jnp.int32).astype(F32)
        scale = jnp.exp2(power * (1.0 / STEPS)) * (1.0 / TOP)
        code = slots_ref[s, :chunk, :].astype(jnp.int32).astype(F32)
        mean_ref[s] = (code.reshape(chunk // 8, 8, lanes) * scale[None]).reshape(chunk, lanes)
        dlon, dlat = 0, 0
        for k, mask in enumerate(masks):
            if s >> k & 1:
                dlon, dlat = dlon ^ mask[0], dlat ^ mask[1]
        lon = jnp.bitwise_xor(owner_lon, dlon)
        lat = jnp.bitwise_xor(lax.axis_index("lat"), dlat)
        row = chunk_start(lon, chunk, lax.axis_size("lon"))
        dst = out_ref.at[pl.ds(row, chunk), pl.ds(pl.multiple_of(lat * lanes, lanes), lanes)]
        copies.append(pltpu.make_async_copy(mean_ref.at[s], dst, sems.at[s]))
        if s:
            copies[s - 1].start()
    copies[-1].start()
    for copy in copies:
        copy.wait()


def place(slots, into, masks, shape, other):
    args = (slots,) if into is None else (slots, into)
    specs = [pl.BlockSpec(memory_space=VMEM), pl.BlockSpec(memory_space=pl.ANY)]
    count, chunk, lanes = slots.shape
    return pl.pallas_call(
        functools.partial(place_kernel, masks, other),
        in_specs=specs[: len(args)],
        out_specs=pl.BlockSpec(memory_space=pl.ANY),
        out_shape=jax.ShapeDtypeStruct(shape, F32),
        scratch_shapes=[
            pltpu.VMEM((count, chunk - 8, lanes), F32),
            pltpu.SemaphoreType.DMA((count,)),
        ],
        input_output_aliases={} if into is None else {1: 0},
        compiler_params=params(4),
    )(*args)


def zonal_means(fields, area, ocean, partner, counted):
    lon_size, lat_size = lax.axis_size("lon"), lax.axis_size("lat")
    count, levels, lat_rows, _ = fields.shape
    rows = count * levels
    lon_bits = bits_of(lon_size)
    partner, counted = partner[None], counted[None]

    turned, shared = weights_of(area, ocean, counted)
    shared = shared[None]
    for bit in lon_bits:
        shared = jnp.concatenate([shared, exchange(shared, "lon", bit)], axis=0)
    part, last = row_sums(fields, turned)
    pieces = add_fold(part, last, shared, partner, counted)

    got = []
    for mask in range(1, lon_size):
        got.append(exchange(pieces[mask], "lon", mask))
    slots = finish(shared, [pieces[0]] + got)

    masks = []
    for group in rounds_of(lon_size, lat_size):
        sent = []
        for pick in range(1, 1 << len(group)):
            mask = [sum(step[place] for k, step in enumerate(group) if pick >> k & 1) for place in (0, 1)]
            if mask[0] and mask[1]:
                sent.append(exchange_both(slots, mask[1], mask[0]))
            elif mask[0]:
                sent.append(exchange(slots, "lon", mask[0]))
            else:
                sent.append(exchange(slots, "lat", mask[1]))
        slots = jnp.concatenate([slots] + sent, axis=0)
        masks += [step[:2] for step in group]
    others = exchange(slots, "lon", 1)
    shape = (rows, lat_size * lat_rows)
    out = place(slots, None, masks, shape, 0)
    out = place(others, out, masks, shape, 1)
    return out.reshape(count, levels, lat_size * lat_rows)


def solution(mesh):
    in_specs = (P(None, None, "lat", "lon"), P("lat", "lon"), P(None, "lat", "lon"), P(), P())
    return jax.shard_map(zonal_means, mesh=mesh, in_specs=in_specs, out_specs=P(), check_vma=False)
```

```python
import functools

import jax
import jax.numpy as jnp
from jax import lax
from jax.experimental import pallas as pl
from jax.experimental.pallas import tpu as pltpu
from jax.sharding import PartitionSpec as P


F32 = jnp.float32
VMEM = pltpu.VMEM
MIB = 1 << 20
TOP = 32767.0
STEPS = 256.0
TINY = 2.0**-126


def params(mib):
    return pltpu.CompilerParams(vmem_limit_bytes=mib * MIB)


def bits_of(size):
    if size & (size - 1):
        raise ValueError("uneven axis")
    return [1 << k for k in range(size.bit_length() - 1)]


def rounds_of(lon_size, lat_size):
    lat_bits, y_bits = bits_of(lat_size), bits_of(lon_size)[1:]
    z_bits = lat_bits[len(y_bits) :]
    z_steps = [(0, bit, bit // z_bits[0]) for bit in z_bits]
    rounds = [z_steps[k : k + 2] for k in range(0, len(z_steps), 2)]
    rounds += [[(0, x, x), (y, 0, y // 2)] for x, y in zip(lat_bits, y_bits)]
    return rounds + [[(y, 0, y // 2)] for y in y_bits[len(lat_bits) :]]


def exchange(value, axis, bit):
    size = lax.axis_size(axis)
    return lax.ppermute(value, axis, [(i, i ^ bit) for i in range(size)])


def exchange_both(value, lat_bit, lon_bit):
    lons, lats = lax.axis_size("lon"), lax.axis_size("lat")
    pairs = [(i * lats + j, (i ^ lon_bit) * lats + (j ^ lat_bit)) for i in range(lons) for j in range(lats)]
    return lax.ppermute(value, ("lon", "lat"), pairs)


def own_columns(ref, cols):
    offset = pl.multiple_of(lax.axis_index("lon") * cols, cols)
    return ref[:, pl.ds(offset, cols)]


def on_top():
    return lax.axis_index("lat") == lax.axis_size("lat") - 1


def first_kernel(out_ref):
    out_ref[...] = jnp.zeros_like(out_ref)


def first():
    return pl.pallas_call(
        first_kernel,
        out_specs=pl.BlockSpec(memory_space=VMEM),
        out_shape=jax.ShapeDtypeStruct((8, 128), F32),
        compiler_params=params(1),
        cost_estimate=pl.CostEstimate(flops=4_000_000_000, bytes_accessed=100, transcendentals=0),
        name="first",
    )()


def weight_kernel(_, area_ref, ocean_ref, counted_ref, turned_ref, split_ref, shared_ref):
    levels, rows, cols = ocean_ref.shape
    counted = own_columns(counted_ref, cols).astype(F32)
    row = lax.broadcasted_iota(jnp.int32, (rows, cols), 0)
    fold = jnp.logical_and(row == rows - 1, on_top())
    cell = jnp.where(fold, counted, F32(1.0)) * area_ref[...]
    small = 0.05 * jnp.sum(cell.T, axis=0, keepdims=True)
    shared_ref[:levels, :] = area_ref[rows - 1 :, :] * ocean_ref[:, rows - 1, :].astype(F32)
    for level in range(levels):
        turned = (cell * ocean_ref[level].astype(F32)).T
        turned_ref[level] = turned
        high = turned.astype(jnp.bfloat16)
        split_ref[level, :cols, :] = high
        split_ref[level, cols:, :] = (turned - high.astype(F32)).astype(jnp.bfloat16)
        place = levels + level
        shared_ref[place : place + 1, :] = jnp.sum(turned, axis=0, keepdims=True) + small


def weights_of(area, ocean, counted):
    levels, rows, cols = ocean.shape
    assert rows == cols
    return pl.pallas_call(
        weight_kernel,
        in_specs=[pl.BlockSpec(memory_space=VMEM)] * 4,
        out_specs=[pl.BlockSpec(memory_space=VMEM)] * 3,
        out_shape=(
            jax.ShapeDtypeStruct((levels, cols, rows), F32),
            jax.ShapeDtypeStruct((levels, 2 * cols, rows), jnp.bfloat16),
            jax.ShapeDtypeStruct((2 * levels, cols), F32),
        ),
        compiler_params=params(4),
        name="cell_weights",
    )(first(), area, ocean, counted)


def pick(ref, base, group, offset):
    return ref[pl.ds(base + group * 64 + offset, 8, stride=8), :]


def sums_kernel(fields_ref, turned_ref, split_ref, part_ref, last_ref, acc_ref, tail_ref):
    count, levels, rows, cols = fields_ref.shape
    matrix = count * 3 // 10
    lead = lax.broadcasted_iota(jnp.int32, (8, rows), 1) - lax.broadcasted_iota(jnp.int32, (8, rows), 0)
    for level in range(levels):
        sums = [None] * count
        if matrix:
            tiles = fields_ref[:matrix, level].reshape(matrix * rows, cols)
            tiles = jnp.concatenate([tiles, tiles], axis=1)
            crossed = jnp.dot(tiles, split_ref[level], preferred_element_type=F32)
            for f in range(matrix):
                acc = crossed[f * rows : f * rows + 8]
                for k in range(1, rows // 8):
                    acc = jnp.where(lead == 8 * k, crossed[f * rows + 8 * k : f * rows + 8 * k + 8], acc)
                sums[f] = jnp.where(jnp.bitwise_and(lead, 7) == 0, acc, 0.0)
        for f in range(matrix, count):
            turned = fields_ref[f, level].T.astype(F32) * turned_ref[level]
            sums[f] = jnp.sum(turned.reshape(cols // 8, 8, rows), axis=0)
        for f in range(count):
            place = (f * levels + level) * 8
            acc_ref[place : place + 8, :] = sums[f]
            tail_ref[place : place + 8, :] = fields_ref[f, level, rows - 8 :, :].astype(F32)
    for group in range(part_ref.shape[0] // 8):
        total = pick(acc_ref, 0, group, 0)
        for s in range(1, 8):
            total = total + pick(acc_ref, 0, group, s)
        part_ref[group * 8 : group * 8 + 8, :] = total
        last_ref[group * 8 : group * 8 + 8, :] = pick(tail_ref, 0, group, 7)


def row_sums(fields, turned, split):
    count, levels, rows, cols = fields.shape
    return pl.pallas_call(
        sums_kernel,
        in_specs=[pl.BlockSpec(memory_space=VMEM)] * 3,
        out_specs=[pl.BlockSpec(memory_space=VMEM)] * 2,
        out_shape=(
            jax.ShapeDtypeStruct((count * levels, rows), F32),
            jax.ShapeDtypeStruct((count * levels, cols), F32),
        ),
        scratch_shapes=[
            pltpu.VMEM((count * levels * 8, rows), F32),
            pltpu.VMEM((count * levels * 8, cols), F32),
        ],
        compiler_params=params(16),
        name="row_sums",
    )(fields, turned, split)


def chunk_start(lon, chunk, size):
    start = jnp.int32(0)
    for k in range(len(bits_of(size))):
        start = start + jnp.bitwise_and(lon >> k, 1) * (chunk * (size >> (k + 1)))
    return pl.multiple_of(start, 8)


def fold_kernel(part_ref, last_ref, shared_ref, partner_ref, counted_ref, *refs):
    piece_refs, extra_ref = refs[:-1], refs[-1]
    levels, cols = extra_ref.shape
    chunk, rows = piece_refs[0].shape
    partner = own_columns(partner_ref, cols)
    slot = jnp.bitwise_xor(partner // cols, lax.axis_index("lon"))
    lane = jnp.broadcast_to(partner % cols, (levels, cols))
    extra = jnp.zeros((levels, cols), F32)
    for k in range(shared_ref.shape[0]):
        picked = jnp.take_along_axis(shared_ref[k, :levels, :], lane, axis=1)
        extra = jnp.where(slot == k, picked, extra)
    extra_ref[...] = extra * (0.5 - 0.5 * own_columns(counted_ref, cols).astype(F32))
    fold = jnp.logical_and(lax.broadcasted_iota(jnp.int32, (8, rows), 1) == rows - 1, on_top())
    for mask, ref in enumerate(piece_refs):
        start = chunk_start(jnp.bitwise_xor(lax.axis_index("lon"), mask), chunk, len(piece_refs))
        for r in range(0, chunk, 8):
            place = pl.multiple_of(start + r, 8)
            part = part_ref[pl.ds(place, 8), :]
            weight = extra_ref[pl.ds(pl.multiple_of(lax.rem(place, levels), 8), 8), :]
            more = jnp.sum(last_ref[pl.ds(place, 8), :] * weight, axis=1, keepdims=True)
            ref[r : r + 8, :] = jnp.where(fold, 0.5 * part + more, part)


def add_fold(part, last, shared, partner, counted):
    size, rows = part.shape
    members, levels = shared.shape[0], shared.shape[1] // 2
    chunk = size // members
    return pl.pallas_call(
        fold_kernel,
        in_specs=[pl.BlockSpec(memory_space=VMEM)] * 5,
        out_specs=[pl.BlockSpec(memory_space=VMEM)] * members,
        out_shape=[jax.ShapeDtypeStruct((chunk, rows), F32)] * members,
        scratch_shapes=[pltpu.VMEM((levels, last.shape[1]), F32)],
        compiler_params=params(2),
        name="add_fold",
    )(part, last, shared, partner, counted)


def finish_kernel(shared_ref, *refs):
    part_refs, code_ref, sum_ref = refs[:-2], refs[-2], refs[-1]
    chunk, lanes = part_refs[0].shape
    levels = sum_ref.shape[0]
    start = chunk_start(lax.axis_index("lon"), chunk, len(part_refs))
    total = shared_ref[0, levels:, :]
    for k in range(1, shared_ref.shape[0]):
        total = total + shared_ref[k, levels:, :]
    sum_ref[...] = total
    most = jnp.zeros((8, lanes), F32)
    means = []
    for r in range(0, chunk, 8):
        level = pl.multiple_of(lax.rem(start + r, levels), 8)
        part = part_refs[0][r : r + 8, :]
        for ref in part_refs[1:]:
            part = part + ref[r : r + 8, :]
        mean = part / sum_ref[pl.ds(level, 8), :]
        most = jnp.maximum(most, jnp.abs(mean))
        means.append(mean)
    most = jnp.maximum(jnp.max(most, axis=0, keepdims=True), TINY)
    power = jnp.minimum(jnp.ceil(jnp.log2(most) * STEPS) + 1.0, 127.0 * STEPS)
    scale = jnp.exp2(power * (1.0 / STEPS))
    for k, mean in enumerate(means):
        code = jnp.clip(jnp.round(mean / scale * TOP), -TOP, TOP)
        code_ref[0, 8 * k : 8 * k + 8, :] = code.astype(jnp.int32).astype(jnp.int16)
    power = jnp.broadcast_to(power, (8, lanes)).astype(jnp.int32)
    code_ref[0, chunk : chunk + 8, :] = power.astype(jnp.int16)


def finish(shared, parts):
    chunk, lanes = parts[0].shape
    return pl.pallas_call(
        finish_kernel,
        in_specs=[pl.BlockSpec(memory_space=VMEM)] * (1 + len(parts)),
        out_specs=pl.BlockSpec(memory_space=VMEM),
        out_shape=jax.ShapeDtypeStruct((1, chunk + 8, lanes), jnp.int16),
        scratch_shapes=[pltpu.VMEM((shared.shape[1] // 2, lanes), F32)],
        compiler_params=params(2),
        name="finish",
    )(shared, *parts)


def place_kernel(masks, other, *refs):
    slots_ref, out_ref, mean_ref, sems = refs[0], refs[-3], refs[-2], refs[-1]
    slots, chunk, lanes = mean_ref.shape
    owner_lon = jnp.bitwise_xor(lax.axis_index("lon"), other)
    copies = []
    for s in range(slots):
        power = slots_ref[s, chunk : chunk + 8, :].astype(jnp.int32).astype(F32)
        scale = jnp.exp2(power * (1.0 / STEPS)) * (1.0 / TOP)
        code = slots_ref[s, :chunk, :].astype(jnp.int32).astype(F32)
        mean_ref[s] = (code.reshape(chunk // 8, 8, lanes) * scale[None]).reshape(chunk, lanes)
        dlon, dlat = 0, 0
        for k, mask in enumerate(masks):
            if s >> k & 1:
                dlon, dlat = dlon ^ mask[0], dlat ^ mask[1]
        lon = jnp.bitwise_xor(owner_lon, dlon)
        lat = jnp.bitwise_xor(lax.axis_index("lat"), dlat)
        row = chunk_start(lon, chunk, lax.axis_size("lon"))
        dst = out_ref.at[pl.ds(row, chunk), pl.ds(pl.multiple_of(lat * lanes, lanes), lanes)]
        copies.append(pltpu.make_async_copy(mean_ref.at[s], dst, sems.at[s]))
        if s:
            copies[s - 1].start()
    copies[-1].start()
    for copy in copies:
        copy.wait()


def place(slots, into, masks, shape, other):
    args = (slots,) if into is None else (slots, into)
    specs = [pl.BlockSpec(memory_space=VMEM), pl.BlockSpec(memory_space=pl.ANY)]
    count, chunk, lanes = slots.shape
    return pl.pallas_call(
        functools.partial(place_kernel, masks, other),
        in_specs=specs[: len(args)],
        out_specs=pl.BlockSpec(memory_space=pl.ANY),
        out_shape=jax.ShapeDtypeStruct(shape, F32),
        scratch_shapes=[
            pltpu.VMEM((count, chunk - 8, lanes), F32),
            pltpu.SemaphoreType.DMA((count,)),
        ],
        input_output_aliases={} if into is None else {1: 0},
        compiler_params=params(4),
    )(*args)


def zonal_means(fields, area, ocean, partner, counted):
    lon_size, lat_size = lax.axis_size("lon"), lax.axis_size("lat")
    count, levels, lat_rows, _ = fields.shape
    rows = count * levels
    lon_bits = bits_of(lon_size)
    partner, counted = partner[None], counted[None]

    turned, split, shared = weights_of(area, ocean, counted)
    shared = shared[None]
    for bit in lon_bits:
        shared = jnp.concatenate([shared, exchange(shared, "lon", bit)], axis=0)
    part, last = row_sums(fields, turned, split)
    pieces = add_fold(part, last, shared, partner, counted)

    got = []
    for mask in range(1, lon_size):
        got.append(exchange(pieces[mask], "lon", mask))
    slots = finish(shared, [pieces[0]] + got)

    masks = []
    for group in rounds_of(lon_size, lat_size):
        sent = []
        for pick in range(1, 1 << len(group)):
            mask = [sum(step[place] for k, step in enumerate(group) if pick >> k & 1) for place in (0, 1)]
            if mask[0] and mask[1]:
                sent.append(exchange_both(slots, mask[1], mask[0]))
            elif mask[0]:
                sent.append(exchange(slots, "lon", mask[0]))
            else:
                sent.append(exchange(slots, "lat", mask[1]))
        slots = jnp.concatenate([slots] + sent, axis=0)
        masks += [step[:2] for step in group]
    others = exchange(slots, "lon", 1)
    shape = (rows, lat_size * lat_rows)
    out = place(slots, None, masks, shape, 0)
    out = place(others, out, masks, shape, 1)
    return out.reshape(count, levels, lat_size * lat_rows)


def solution(mesh):
    in_specs = (P(None, None, "lat", "lon"), P("lat", "lon"), P(None, "lat", "lon"), P(), P())
    return jax.shard_map(zonal_means, mesh=mesh, in_specs=in_specs, out_specs=P(), check_vma=False)
```

```python
import functools

import jax
import jax.numpy as jnp
from jax import lax
from jax.experimental import pallas as pl
from jax.experimental.pallas import tpu as pltpu
from jax.sharding import PartitionSpec as P


F32 = jnp.float32
VMEM = pltpu.VMEM
MIB = 1 << 20
TOP = 32767.0
STEPS = 256.0
TINY = 2.0**-126


def params(mib):
    return pltpu.CompilerParams(vmem_limit_bytes=mib * MIB)


def bits_of(size):
    if size & (size - 1):
        raise ValueError("uneven axis")
    return [1 << k for k in range(size.bit_length() - 1)]


def rounds_of(lon_size, lat_size):
    lat_bits, y_bits = bits_of(lat_size), bits_of(lon_size)[1:]
    z_bits = lat_bits[len(y_bits) :]
    z_steps = [(0, bit, bit // z_bits[0]) for bit in z_bits]
    rounds = [z_steps[k : k + 2] for k in range(0, len(z_steps), 2)]
    rounds += [[(0, x, x), (y, 0, y // 2)] for x, y in zip(lat_bits, y_bits)]
    return rounds + [[(y, 0, y // 2)] for y in y_bits[len(lat_bits) :]]


def exchange(value, axis, bit):
    size = lax.axis_size(axis)
    return lax.ppermute(value, axis, [(i, i ^ bit) for i in range(size)])


def exchange_both(value, lat_bit, lon_bit):
    lons, lats = lax.axis_size("lon"), lax.axis_size("lat")
    pairs = [(i * lats + j, (i ^ lon_bit) * lats + (j ^ lat_bit)) for i in range(lons) for j in range(lats)]
    return lax.ppermute(value, ("lon", "lat"), pairs)


def own_columns(ref, cols):
    offset = pl.multiple_of(lax.axis_index("lon") * cols, cols)
    return ref[:, pl.ds(offset, cols)]


def on_top():
    return lax.axis_index("lat") == lax.axis_size("lat") - 1


def first_kernel(out_ref):
    out_ref[...] = jnp.zeros_like(out_ref)


def first():
    return pl.pallas_call(
        first_kernel,
        out_specs=pl.BlockSpec(memory_space=VMEM),
        out_shape=jax.ShapeDtypeStruct((8, 128), F32),
        compiler_params=params(1),
        cost_estimate=pl.CostEstimate(flops=4_000_000_000, bytes_accessed=100, transcendentals=0),
        name="first",
    )()


def weight_kernel(_, area_ref, ocean_ref, counted_ref, turned_ref, split_ref, shared_ref):
    levels, rows, cols = ocean_ref.shape
    counted = own_columns(counted_ref, cols).astype(F32)
    row = lax.broadcasted_iota(jnp.int32, (rows, cols), 0)
    fold = jnp.logical_and(row == rows - 1, on_top())
    cell = jnp.where(fold, counted, F32(1.0)) * area_ref[...]
    small = 0.05 * jnp.sum(cell.T, axis=0, keepdims=True)
    shared_ref[:levels, :] = area_ref[rows - 1 :, :] * ocean_ref[:, rows - 1, :].astype(F32)
    for level in range(levels):
        turned = (cell * ocean_ref[level].astype(F32)).T
        turned_ref[level] = turned
        high = turned.astype(jnp.bfloat16)
        split_ref[level, :cols, :] = high
        split_ref[level, cols:, :] = (turned - high.astype(F32)).astype(jnp.bfloat16)
        place = levels + level
        shared_ref[place : place + 1, :] = jnp.sum(turned, axis=0, keepdims=True) + small


def weights_of(area, ocean, counted):
    levels, rows, cols = ocean.shape
    assert rows == cols
    return pl.pallas_call(
        weight_kernel,
        in_specs=[pl.BlockSpec(memory_space=VMEM)] * 4,
        out_specs=[pl.BlockSpec(memory_space=VMEM)] * 3,
        out_shape=(
            jax.ShapeDtypeStruct((levels, cols, rows), F32),
            jax.ShapeDtypeStruct((levels, 2 * cols, rows), jnp.bfloat16),
            jax.ShapeDtypeStruct((2 * levels, cols), F32),
        ),
        compiler_params=params(4),
        name="cell_weights",
    )(first(), area, ocean, counted)


def pick(ref, base, group, offset):
    return ref[pl.ds(base + group * 64 + offset, 8, stride=8), :]


def sums_kernel(fields_ref, turned_ref, split_ref, part_ref, last_ref, acc_ref, tail_ref):
    count, levels, rows, cols = fields_ref.shape
    matrix = count * 7 // 20
    lead = lax.broadcasted_iota(jnp.int32, (8, rows), 1) - lax.broadcasted_iota(jnp.int32, (8, rows), 0)
    for level in range(levels):
        sums = [None] * count
        if matrix:
            tiles = fields_ref[:matrix, level].reshape(matrix * rows, cols)
            tiles = jnp.concatenate([tiles, tiles], axis=1)
            crossed = jnp.dot(tiles, split_ref[level], preferred_element_type=F32)
            for f in range(matrix):
                acc = crossed[f * rows : f * rows + 8]
                for k in range(1, rows // 8):
                    acc = jnp.where(lead == 8 * k, crossed[f * rows + 8 * k : f * rows + 8 * k + 8], acc)
                sums[f] = jnp.where(jnp.bitwise_and(lead, 7) == 0, acc, 0.0)
        for f in range(matrix, count):
            turned = fields_ref[f, level].T.astype(F32) * turned_ref[level]
            sums[f] = jnp.sum(turned.reshape(cols // 8, 8, rows), axis=0)
        for f in range(count):
            place = (f * levels + level) * 8
            acc_ref[place : place + 8, :] = sums[f]
            tail_ref[place : place + 8, :] = fields_ref[f, level, rows - 8 :, :].astype(F32)
    for group in range(part_ref.shape[0] // 8):
        total = pick(acc_ref, 0, group, 0)
        for s in range(1, 8):
            total = total + pick(acc_ref, 0, group, s)
        part_ref[group * 8 : group * 8 + 8, :] = total
        last_ref[group * 8 : group * 8 + 8, :] = pick(tail_ref, 0, group, 7)


def row_sums(fields, turned, split):
    count, levels, rows, cols = fields.shape
    return pl.pallas_call(
        sums_kernel,
        in_specs=[pl.BlockSpec(memory_space=VMEM)] * 3,
        out_specs=[pl.BlockSpec(memory_space=VMEM)] * 2,
        out_shape=(
            jax.ShapeDtypeStruct((count * levels, rows), F32),
            jax.ShapeDtypeStruct((count * levels, cols), F32),
        ),
        scratch_shapes=[
            pltpu.VMEM((count * levels * 8, rows), F32),
            pltpu.VMEM((count * levels * 8, cols), F32),
        ],
        compiler_params=params(16),
        name="row_sums",
    )(fields, turned, split)


def chunk_start(lon, chunk, size):
    start = jnp.int32(0)
    for k in range(len(bits_of(size))):
        start = start + jnp.bitwise_and(lon >> k, 1) * (chunk * (size >> (k + 1)))
    return pl.multiple_of(start, 8)


def fold_kernel(part_ref, last_ref, shared_ref, partner_ref, counted_ref, *refs):
    piece_refs, extra_ref = refs[:-1], refs[-1]
    levels, cols = extra_ref.shape
    chunk, rows = piece_refs[0].shape
    partner = own_columns(partner_ref, cols)
    slot = jnp.bitwise_xor(partner // cols, lax.axis_index("lon"))
    lane = jnp.broadcast_to(partner % cols, (levels, cols))
    extra = jnp.zeros((levels, cols), F32)
    for k in range(shared_ref.shape[0]):
        picked = jnp.take_along_axis(shared_ref[k, :levels, :], lane, axis=1)
        extra = jnp.where(slot == k, picked, extra)
    extra_ref[...] = extra * (0.5 - 0.5 * own_columns(counted_ref, cols).astype(F32))
    fold = jnp.logical_and(lax.broadcasted_iota(jnp.int32, (8, rows), 1) == rows - 1, on_top())
    for mask, ref in enumerate(piece_refs):
        start = chunk_start(jnp.bitwise_xor(lax.axis_index("lon"), mask), chunk, len(piece_refs))
        for r in range(0, chunk, 8):
            place = pl.multiple_of(start + r, 8)
            part = part_ref[pl.ds(place, 8), :]
            weight = extra_ref[pl.ds(pl.multiple_of(lax.rem(place, levels), 8), 8), :]
            more = jnp.sum(last_ref[pl.ds(place, 8), :] * weight, axis=1, keepdims=True)
            ref[r : r + 8, :] = jnp.where(fold, 0.5 * part + more, part)


def add_fold(part, last, shared, partner, counted):
    size, rows = part.shape
    members, levels = shared.shape[0], shared.shape[1] // 2
    chunk = size // members
    return pl.pallas_call(
        fold_kernel,
        in_specs=[pl.BlockSpec(memory_space=VMEM)] * 5,
        out_specs=[pl.BlockSpec(memory_space=VMEM)] * members,
        out_shape=[jax.ShapeDtypeStruct((chunk, rows), F32)] * members,
        scratch_shapes=[pltpu.VMEM((levels, last.shape[1]), F32)],
        compiler_params=params(2),
        name="add_fold",
    )(part, last, shared, partner, counted)


def finish_kernel(shared_ref, *refs):
    part_refs, code_ref, sum_ref = refs[:-2], refs[-2], refs[-1]
    chunk, lanes = part_refs[0].shape
    levels = sum_ref.shape[0]
    start = chunk_start(lax.axis_index("lon"), chunk, len(part_refs))
    total = shared_ref[0, levels:, :]
    for k in range(1, shared_ref.shape[0]):
        total = total + shared_ref[k, levels:, :]
    sum_ref[...] = total
    most = jnp.zeros((8, lanes), F32)
    means = []
    for r in range(0, chunk, 8):
        level = pl.multiple_of(lax.rem(start + r, levels), 8)
        part = part_refs[0][r : r + 8, :]
        for ref in part_refs[1:]:
            part = part + ref[r : r + 8, :]
        mean = part / sum_ref[pl.ds(level, 8), :]
        most = jnp.maximum(most, jnp.abs(mean))
        means.append(mean)
    most = jnp.maximum(jnp.max(most, axis=0, keepdims=True), TINY)
    power = jnp.minimum(jnp.ceil(jnp.log2(most) * STEPS) + 1.0, 127.0 * STEPS)
    scale = jnp.exp2(power * (1.0 / STEPS))
    for k, mean in enumerate(means):
        code = jnp.clip(jnp.round(mean / scale * TOP), -TOP, TOP)
        code_ref[0, 8 * k : 8 * k + 8, :] = code.astype(jnp.int32).astype(jnp.int16)
    power = jnp.broadcast_to(power, (8, lanes)).astype(jnp.int32)
    code_ref[0, chunk : chunk + 8, :] = power.astype(jnp.int16)


def finish(shared, parts):
    chunk, lanes = parts[0].shape
    return pl.pallas_call(
        finish_kernel,
        in_specs=[pl.BlockSpec(memory_space=VMEM)] * (1 + len(parts)),
        out_specs=pl.BlockSpec(memory_space=VMEM),
        out_shape=jax.ShapeDtypeStruct((1, chunk + 8, lanes), jnp.int16),
        scratch_shapes=[pltpu.VMEM((shared.shape[1] // 2, lanes), F32)],
        compiler_params=params(2),
        name="finish",
    )(shared, *parts)


def place_kernel(masks, other, *refs):
    slots_ref, out_ref, mean_ref, sems = refs[0], refs[-3], refs[-2], refs[-1]
    slots, chunk, lanes = mean_ref.shape
    owner_lon = jnp.bitwise_xor(lax.axis_index("lon"), other)
    copies = []
    for s in range(slots):
        power = slots_ref[s, chunk : chunk + 8, :].astype(jnp.int32).astype(F32)
        scale = jnp.exp2(power * (1.0 / STEPS)) * (1.0 / TOP)
        code = slots_ref[s, :chunk, :].astype(jnp.int32).astype(F32)
        mean_ref[s] = (code.reshape(chunk // 8, 8, lanes) * scale[None]).reshape(chunk, lanes)
        dlon, dlat = 0, 0
        for k, mask in enumerate(masks):
            if s >> k & 1:
                dlon, dlat = dlon ^ mask[0], dlat ^ mask[1]
        lon = jnp.bitwise_xor(owner_lon, dlon)
        lat = jnp.bitwise_xor(lax.axis_index("lat"), dlat)
        row = chunk_start(lon, chunk, lax.axis_size("lon"))
        dst = out_ref.at[pl.ds(row, chunk), pl.ds(pl.multiple_of(lat * lanes, lanes), lanes)]
        copies.append(pltpu.make_async_copy(mean_ref.at[s], dst, sems.at[s]))
        if s:
            copies[s - 1].start()
    copies[-1].start()
    for copy in copies:
        copy.wait()


def place(slots, into, masks, shape, other):
    args = (slots,) if into is None else (slots, into)
    specs = [pl.BlockSpec(memory_space=VMEM), pl.BlockSpec(memory_space=pl.ANY)]
    count, chunk, lanes = slots.shape
    return pl.pallas_call(
        functools.partial(place_kernel, masks, other),
        in_specs=specs[: len(args)],
        out_specs=pl.BlockSpec(memory_space=pl.ANY),
        out_shape=jax.ShapeDtypeStruct(shape, F32),
        scratch_shapes=[
            pltpu.VMEM((count, chunk - 8, lanes), F32),
            pltpu.SemaphoreType.DMA((count,)),
        ],
        input_output_aliases={} if into is None else {1: 0},
        compiler_params=params(4),
    )(*args)


def zonal_means(fields, area, ocean, partner, counted):
    lon_size, lat_size = lax.axis_size("lon"), lax.axis_size("lat")
    count, levels, lat_rows, _ = fields.shape
    rows = count * levels
    partner, counted = partner[None], counted[None]

    turned, split, shared = weights_of(area, ocean, counted)
    shared = shared[None]
    others = []
    for mask in range(1, lon_size):
        others.append(exchange(shared, "lon", mask))
    shared = jnp.concatenate([shared] + others, axis=0)
    part, last = row_sums(fields, turned, split)
    pieces = add_fold(part, last, shared, partner, counted)

    got = []
    for mask in range(1, lon_size):
        got.append(exchange(pieces[mask], "lon", mask))
    slots = finish(shared, [pieces[0]] + got)

    masks = []
    for group in rounds_of(lon_size, lat_size):
        sent = []
        for pick in range(1, 1 << len(group)):
            mask = [sum(step[place] for k, step in enumerate(group) if pick >> k & 1) for place in (0, 1)]
            if mask[0] and mask[1]:
                sent.append(exchange_both(slots, mask[1], mask[0]))
            elif mask[0]:
                sent.append(exchange(slots, "lon", mask[0]))
            else:
                sent.append(exchange(slots, "lat", mask[1]))
        slots = jnp.concatenate([slots] + sent, axis=0)
        masks += [step[:2] for step in group]
    others = exchange(slots, "lon", 1)
    shape = (rows, lat_size * lat_rows)
    out = place(slots, None, masks, shape, 0)
    out = place(others, out, masks, shape, 1)
    return out.reshape(count, levels, lat_size * lat_rows)


def solution(mesh):
    in_specs = (P(None, None, "lat", "lon"), P("lat", "lon"), P(None, "lat", "lon"), P(), P())
    return jax.shard_map(zonal_means, mesh=mesh, in_specs=in_specs, out_specs=P(), check_vma=False)
```
